32 devices in a mesh: dp: 32 (over z, y, x, core).
Axes of the slice: x: 2, y: 2, z: 4, core: 2. Of those that a mesh axis runs over, the one named last changes fastest.
Arguments:
- features: bfloat16 [256, 128, 1024], P('dp'), may hold values from -16 to 16
- ln_gain: float32 [1024], replicated, may hold values from 0.5 to 1.5
- w_query: bfloat16 [1024, 1024], replicated, may hold values from -0.1875 to 0.1875
- w_key: bfloat16 [1024, 1024], replicated, may hold values from -0.1875 to 0.1875
- w_value: bfloat16 [1024, 1024], replicated, may hold values from -0.1875 to 0.1875
- w_out: bfloat16 [1024, 1024], replicated, may hold values from -0.1875 to 0.1875
- text_raw: bfloat16 [256, 1024], P('dp'), may hold values from -0.35 to 0.35
Outputs:
- loss: float32 [], replicated
- text_grad: float32 [256, 1024], P('dp')
- w_out_grad: bfloat16 [1024, 1024], replicated
The draws below stay inside these ranges and needn't reach their ends.
All inputs are finite; a program needn't handle non-finite values.
Results may differ from the reference program's by a relative error of at most 0.009.
Values may be sent and summed in bfloat16 or wider, within the bound.
No kernel may reach another device: no remote copies, remote signals or barrier semaphores. Data moves between devices by JAX's collectives and lax.ppermute only.
A program may use at most 128 MiB of HBM per device.

```python
import jax
import jax.numpy as jnp
from jax import lax

D = 1024
HEADS = 16
PATCHES = 127
BATCH = 256


def unit_noise(rng_key, shape):
    return jax.random.truncated_normal(rng_key, -4.0, 4.0, shape, jnp.float32)


def paired_rows(key):
    folded = jax.random.fold_in(key, 1031)
    streams = jax.random.split(folded, 7)
    common = unit_noise(streams[0], (1, D))
    shared = unit_noise(streams[1], (BATCH, D))
    image_noise = unit_noise(streams[2], (BATCH, D))
    text_noise = unit_noise(streams[3], (BATCH, D))
    order = jax.random.permutation(streams[6], BATCH).astype(jnp.int32)
    partner = jnp.zeros((BATCH,), jnp.int32).at[order].set(jnp.roll(order, -1))
    mate_rows = shared[partner]
    ramp = jnp.arange(BATCH, dtype=jnp.float32)[:, None] / BATCH
    image_scale = jax.random.uniform(streams[4], (BATCH, 1), jnp.float32, 0.3, 0.7)
    text_scale = jax.random.uniform(streams[5], (BATCH, 1), jnp.float32, 0.0, 0.9)
    noise_scale = 0.4 + 1.6 * ramp
    class_rows = image_scale * common + shared + 0.7 * mate_rows + noise_scale * image_noise
    text_rows = 0.03125 * (text_scale * common + shared + 0.8 * text_noise)
    return (class_rows, text_rows)


def draw_features(key, part):
    class_rows, text_rows = paired_rows(key)
    patch_rows = unit_noise(jax.random.fold_in(key, 2063), (BATCH, PATCHES, D))
    return jnp.concatenate([class_rows[:, None, :], patch_rows], axis=1).astype(jnp.bfloat16)


def draw_text_raw(key, part):
    class_rows, text_rows = paired_rows(key)
    return text_rows.astype(jnp.bfloat16)


def normal_values(key, extent, scale, bound, kind=jnp.bfloat16):
    entries = scale * jax.random.normal(key, extent, jnp.float32)
    return jnp.clip(entries, min=-bound, max=bound).astype(kind)


def setup_inputs(seed: int = 0) -> dict:
    key_of = jax.random.split(jax.random.key(seed), 8)
    return {
        "features": draw_features(jax.random.fold_in(key_of[7], 71), 0),
        "ln_gain": jnp.clip(1.0 + 0.1 * jax.random.normal(key_of[1], (D,), jnp.float32), 0.5, 1.5),
        "w_query": normal_values(key_of[2], (D, D), D ** -0.5, 0.1875),
        "w_key": normal_values(key_of[3], (D, D), D ** -0.5, 0.1875),
        "w_value": normal_values(key_of[4], (D, D), D ** -0.5, 0.1875),
        "w_out": normal_values(key_of[5], (D, D), D ** -0.5, 0.1875),
        "text_raw": draw_text_raw(jax.random.fold_in(key_of[7], 71), 0),
    }


inv_temp = 1.0 / 0.07
attn_temp = 8.0
epsilon = 1e-06

def layer_norm(inputs, gain):
    center = inputs - lax.optimization_barrier(jnp.mean(inputs, axis=-1, keepdims=True))
    spread = lax.optimization_barrier(jnp.mean(center * center, axis=-1, keepdims=True))
    return center * lax.rsqrt(spread + epsilon) * gain

def unit_heads(proj, heads):
    shaped = proj.reshape(proj.shape[0], proj.shape[1], heads, -1)
    return (shaped * lax.rsqrt(lax.optimization_barrier(jnp.sum(shaped * shaped, axis=-1, keepdims=True)) + epsilon)).astype(jnp.bfloat16)

def embed(feats, ln_gain, w_query, w_key, w_value, w_out):
    images, tokens, width = feats.shape
    inputs = feats.astype(jnp.float32)
    normed = layer_norm(inputs, ln_gain).astype(jnp.bfloat16).reshape(images * tokens, width)
    query = unit_heads(jnp.dot(normed, w_query, preferred_element_type=jnp.float32).reshape(images, tokens, width), HEADS)
    key_heads = unit_heads(jnp.dot(normed, w_key, preferred_element_type=jnp.float32).reshape(images, tokens, width), HEADS)
    value_heads = jnp.dot(normed, w_value, preferred_element_type=jnp.float32).reshape(images, tokens, HEADS, -1).astype(jnp.bfloat16)
    scores = attn_temp * jnp.einsum('bqhd,bkhd->bhqk', query.astype(jnp.float32), key_heads.astype(jnp.float32))
    expo = jnp.exp(scores)
    weights = (expo / lax.optimization_barrier(jnp.sum(expo, axis=-1, keepdims=True))).astype(jnp.bfloat16).astype(jnp.float32)
    pooled = weights[:, :, 0, :] + lax.optimization_barrier(jnp.mean(weights[:, :, 1:, :], axis=2))
    abar = jnp.einsum('bhk,bkhd->bhd', pooled, value_heads.astype(jnp.float32), precision=lax.Precision.HIGHEST)
    abar = abar.reshape(images, width).astype(jnp.bfloat16)
    xbar = inputs[:, 0, :] + lax.optimization_barrier(jnp.mean(inputs[:, 1:, :], axis=1))
    emb = xbar + jnp.dot(abar, w_out, preferred_element_type=jnp.float32)
    return (emb, abar)

def reference(features, ln_gain, w_query, w_key, w_value, w_out, text_raw):

    def one_image(single):
        return embed(single[None], ln_gain, w_query, w_key, w_value, w_out)
    emb, abar = lax.map(one_image, features)
    emb = emb.reshape(BATCH, D)
    abar = abar.reshape(BATCH, D)
    emb_norm = jnp.sqrt(lax.optimization_barrier(jnp.sum(emb * emb, axis=1, keepdims=True)) + epsilon)
    img_f = emb / emb_norm
    img_u = img_f.astype(jnp.bfloat16)
    text32 = text_raw.astype(jnp.float32)
    txt_norm = jnp.sqrt(lax.optimization_barrier(jnp.sum(text32 * text32, axis=1, keepdims=True)) + epsilon)
    txt_f = text32 / txt_norm
    txt_u = txt_f.astype(jnp.bfloat16)
    logits = inv_temp * jnp.dot(img_u, txt_u.T, preferred_element_type=jnp.float32)
    exp_logits = jnp.exp(logits)
    rowsum = lax.optimization_barrier(jnp.sum(exp_logits, axis=1))
    colsum = lax.optimization_barrier(jnp.sum(exp_logits, axis=0))
    diag_logit = jnp.diagonal(logits)
    loss = (jnp.sum(jnp.log(rowsum) - diag_logit) + jnp.sum(jnp.log(colsum) - diag_logit)) / (2.0 * BATCH)
    delta = 0.5 * (exp_logits / rowsum[:, None] + exp_logits / colsum[None, :]) - jnp.eye(BATCH, dtype=jnp.float32)
    delta = delta.astype(jnp.bfloat16)
    grad_img = inv_temp * jnp.dot(delta, txt_u, preferred_element_type=jnp.float32)
    grad_txt = inv_temp * jnp.dot(delta.T, img_u, preferred_element_type=jnp.float32)
    text_grad = (grad_txt - txt_f * lax.optimization_barrier(jnp.sum(txt_f * grad_txt, axis=1, keepdims=True))) / txt_norm
    emb_grad = (grad_img - img_f * lax.optimization_barrier(jnp.sum(img_f * grad_img, axis=1, keepdims=True))) / emb_norm
    w_out_grad = jnp.dot(abar.astype(jnp.float32).T, emb_grad, precision=lax.Precision.HIGHEST).astype(jnp.bfloat16)
    return (loss, text_grad, w_out_grad)
```

```python
import functools

import jax
import jax.numpy as jnp
from jax import lax
from jax.experimental import pallas as pl
from jax.experimental.pallas import tpu as pltpu
from jax.sharding import PartitionSpec as P

HEADS = 16
LANES = 128
GROUP = 256

inv_temp = 1.0 / 0.07
attn_temp = 8.0
epsilon = 1e-06
log2e = 1.4426950408889634


def fdot(a, b, dims):
    return lax.dot_general(a, b, (dims, ((), ())), preferred_element_type=jnp.float32)


def split_bf16(x):
    hi = x.astype(jnp.bfloat16)
    lo = (x - hi.astype(jnp.float32)).astype(jnp.bfloat16)
    return hi, lo


def embed_kernel(
    feat_hbm,
    gain_ref,
    wq_hbm,
    wk_hbm,
    wv_hbm,
    wo_hbm,
    text_ref,
    out_ref,
    feat,
    wq,
    wk,
    wv,
    wo,
    normed,
    qn,
    kn,
    pooled,
    pn_hi,
    pn_lo,
    xbar,
    feat_sem,
    wqk_sem,
    wvo_sem,
):
    images, tokens, width = feat.shape
    groups = width // GROUP
    head = width // HEADS
    rows = images * tokens

    feat_copies = [
        pltpu.make_async_copy(feat_hbm.at[b], feat.at[b], feat_sem.at[b]) for b in range(images)
    ]
    wqk_copies = []
    for g in range(groups):
        cols = pl.ds(g * GROUP, GROUP)
        wqk_copies.append(
            (
                pltpu.make_async_copy(wq_hbm.at[:, cols], wq.at[:, cols], wqk_sem.at[2 * g]),
                pltpu.make_async_copy(wk_hbm.at[:, cols], wk.at[:, cols], wqk_sem.at[2 * g + 1]),
            )
        )
    wv_copy = pltpu.make_async_copy(wv_hbm, wv, wvo_sem.at[0])
    wo_copy = pltpu.make_async_copy(wo_hbm, wo, wvo_sem.at[1])
    for c in feat_copies:
        c.start()
    for a, b in wqk_copies:
        a.start()
        b.start()
    wv_copy.start()
    wo_copy.start()

    text32 = text_ref[...].astype(jnp.float32)
    txt_norm = jnp.sqrt(jnp.sum(text32 * text32, axis=1, keepdims=True) + epsilon)
    out_ref[:, 0:width] = (text32 / txt_norm).astype(jnp.bfloat16)

    gain = gain_ref[...]
    for b in range(images):
        feat_copies[b].wait()
        x = feat[b].astype(jnp.float32)
        total = jnp.sum(x, axis=0, keepdims=True)
        first = x[0:1, :]
        xbar[b : b + 1, :] = first + (total - first) * (1.0 / (tokens - 1))
        center = x - jnp.mean(x, axis=-1, keepdims=True)
        spread = jnp.mean(center * center, axis=-1, keepdims=True)
        normed[b * tokens : (b + 1) * tokens, :] = (
            center * lax.rsqrt(spread + epsilon) * gain
        ).astype(jnp.bfloat16)

    r_id = lax.broadcasted_iota(jnp.int32, (GROUP, GROUP), 0) // head
    c_id = lax.broadcasted_iota(jnp.int32, (GROUP, GROUP), 1) // head
    block_ones = jnp.where(r_id == c_id, 1.0, 0.0).astype(jnp.bfloat16)
    lane = lax.broadcasted_iota(jnp.int32, (1, LANES), 1)
    left = jnp.where(lane < head, 1.0, 0.0).astype(jnp.bfloat16)
    right = jnp.where(lane < head, 0.0, 1.0).astype(jnp.bfloat16)
    share = jnp.where(
        lax.broadcasted_iota(jnp.int32, (1, tokens), 1) == 0, 1.0, 1.0 / (tokens - 1)
    )
    head_lane = lax.broadcasted_iota(jnp.int32, (tokens, LANES), 1)

    def unit(w, g, dst):
        cols = slice(g * GROUP, (g + 1) * GROUP)
        proj = fdot(normed[...], w[:, cols], ((1,), (0,)))
        squares = fdot((proj * proj).astype(jnp.bfloat16), block_ones, ((1,), (0,)))
        dst[:, cols] = (proj * lax.rsqrt(squares + epsilon)).astype(jnp.bfloat16)

    def attend(g, b):
        here = slice(b * tokens, (b + 1) * tokens)
        for t in range(g * GROUP // LANES, (g + 1) * GROUP // LANES):
            cols = slice(t * LANES, (t + 1) * LANES)
            k_pair = kn[here, cols]
            stacked = jnp.concatenate([k_pair * left, k_pair * right], axis=0)
            scores = fdot(stacked, qn[here, cols], ((1,), (1,)))
            expo = jnp.exp2(scores * (attn_temp * log2e))
            for j in range(2):
                e = expo[j * tokens : (j + 1) * tokens, :]
                scale = share / jnp.sum(e, axis=0, keepdims=True)
                mass = jnp.sum(e * scale, axis=1, keepdims=True)
                old = pooled[b]
                pooled[b] = jnp.where(head_lane == 2 * t + j, mass, old)

    for b in range(images):
        pooled[b] = jnp.zeros((tokens, LANES), jnp.float32)

    for g in range(groups):
        wqk_copies[g][0].wait()
        unit(wq, g, qn)
        wqk_copies[g][1].wait()
        unit(wk, g, kn)
        for b in range(images):
            attend(g, b)

    for b in range(images):
        hi, lo = split_bf16(jnp.transpose(pooled[b])[0:HEADS, :])
        both = jnp.concatenate([hi, lo], axis=0)
        pn = fdot(both, normed[b * tokens : (b + 1) * tokens, :], ((1,), (0,)))
        pn = pn[0:HEADS, :] + pn[HEADS : 2 * HEADS, :]
        hi, lo = split_bf16(pn)
        pn_hi[b * HEADS : (b + 1) * HEADS, :] = hi
        pn_lo[b * HEADS : (b + 1) * HEADS, :] = lo

    wv_copy.wait()
    full = fdot(pn_hi[...], wv[...], ((1,), (0,))) + fdot(pn_lo[...], wv[...], ((1,), (0,)))
    full = full.reshape(images, HEADS, width)
    h_id = lax.broadcasted_iota(jnp.int32, (images, HEADS, width), 1)
    l_id = lax.broadcasted_iota(jnp.int32, (images, HEADS, width), 2) // head
    abar = jnp.sum(jnp.where(h_id == l_id, full, 0.0), axis=1).astype(jnp.bfloat16)

    wo_copy.wait()
    emb = xbar[...] + fdot(abar, wo[...], ((1,), (0,)))
    emb_norm = jnp.sqrt(jnp.sum(emb * emb, axis=1, keepdims=True) + epsilon)
    out_ref[:, width : 2 * width] = (emb / emb_norm).astype(jnp.bfloat16)
    out_ref[:, 2 * width : 3 * width] = (abar.astype(jnp.float32) / emb_norm).astype(jnp.bfloat16)


def embed_call(features, ln_gain, w_query, w_key, w_value, w_out, text_raw):
    images, tokens, width = features.shape
    rows = images * tokens
    hbm = pl.BlockSpec(memory_space=pl.ANY)
    vmem = pl.BlockSpec(memory_space=pltpu.VMEM)
    weight = pltpu.VMEM((width, width), jnp.bfloat16)
    tall = pltpu.VMEM((rows, width), jnp.bfloat16)
    return pl.pallas_call(
        embed_kernel,
        name="embed",
        out_shape=jax.ShapeDtypeStruct((images, 3 * width), jnp.bfloat16),
        in_specs=[hbm, vmem, hbm, hbm, hbm, hbm, vmem],
        out_specs=vmem,
        scratch_shapes=[
            pltpu.VMEM((images, tokens, width), jnp.bfloat16),
            weight,
            weight,
            weight,
            weight,
            tall,
            tall,
            tall,
            pltpu.VMEM((images, tokens, LANES), jnp.float32),
            pltpu.VMEM((images * HEADS, width), jnp.bfloat16),
            pltpu.VMEM((images * HEADS, width), jnp.bfloat16),
            pltpu.VMEM((images, width), jnp.float32),
            pltpu.SemaphoreType.DMA((images,)),
            pltpu.SemaphoreType.DMA((2 * width // GROUP,)),
            pltpu.SemaphoreType.DMA((2,)),
        ],
        compiler_params=pltpu.CompilerParams(vmem_limit_bytes=48 * 1024 * 1024),
    )(features, ln_gain.reshape(1, width), w_query, w_key, w_value, w_out, text_raw)


def contrast(txt, img, abn):
    total, width = txt.shape
    logits = inv_temp * fdot(img, txt, ((1,), (1,)))
    row_id = lax.broadcasted_iota(jnp.int32, (total, total), 0)
    col_id = lax.broadcasted_iota(jnp.int32, (total, total), 1)
    eye = row_id == col_id
    expo = jnp.exp(logits)
    rowsum = jnp.sum(expo, axis=1, keepdims=True)
    colsum = jnp.sum(expo, axis=0, keepdims=True)
    diag = jnp.sum(jnp.where(eye, logits, 0.0), axis=1, keepdims=True)
    loss = (
        jnp.sum(jnp.log(rowsum) - diag, axis=0, keepdims=True)
        + jnp.sum(jnp.log(colsum), axis=1, keepdims=True)
        - jnp.sum(diag, axis=0, keepdims=True)
    ) / (2.0 * total)
    delta = 0.5 * (expo / rowsum + expo / colsum) - jnp.where(eye, 1.0, 0.0)
    delta = delta.astype(jnp.bfloat16)
    grad_img = inv_temp * fdot(delta, txt, ((1,), (0,)))
    img32 = img.astype(jnp.float32)
    along = jnp.sum(img32 * grad_img, axis=1, keepdims=True)
    hi, lo = split_bf16(grad_img - img32 * along)
    w_out_grad = fdot(abn, hi, ((0,), (0,))) + fdot(abn, lo, ((0,), (0,)))
    return loss, delta, w_out_grad.astype(jnp.bfloat16)


def text_back(text_raw, grad_txt):
    text32 = text_raw.astype(jnp.float32)
    txt_norm = jnp.sqrt(jnp.sum(text32 * text32, axis=1, keepdims=True) + epsilon)
    txt_f = text32 / txt_norm
    return (grad_txt - txt_f * jnp.sum(txt_f * grad_txt, axis=1, keepdims=True)) / txt_norm


def contrast_kernel(place_ref, all_ref, text_ref, loss_ref, text_grad_ref, w_grad_ref, grad_txt):
    images, width = text_ref.shape
    txt = all_ref[:, 0:width]
    img = all_ref[:, width : 2 * width]
    abn = all_ref[:, 2 * width : 3 * width]
    loss, delta, w_out_grad = contrast(txt, img, abn)
    loss_ref[...] = loss
    w_grad_ref[...] = w_out_grad
    grad_txt[...] = inv_temp * fdot(delta, img, ((0,), (0,)))
    own = grad_txt[pl.ds(pl.multiple_of(place_ref[0] * images, images), images), :]
    text_grad_ref[...] = text_back(text_ref[...], own)


def contrast_call(place, gathered, text_raw):
    total = gathered.shape[0]
    images, width = text_raw.shape
    vmem = pl.BlockSpec(memory_space=pltpu.VMEM)
    return pl.pallas_call(
        contrast_kernel,
        name="contrast",
        out_shape=(
            jax.ShapeDtypeStruct((1, 1), jnp.float32),
            jax.ShapeDtypeStruct((images, width), jnp.float32),
            jax.ShapeDtypeStruct((width, width), jnp.bfloat16),
        ),
        in_specs=[pl.BlockSpec(memory_space=pltpu.SMEM), vmem, vmem],
        out_specs=(vmem, vmem, vmem),
        scratch_shapes=[pltpu.VMEM((total, width), jnp.float32)],
        compiler_params=pltpu.CompilerParams(vmem_limit_bytes=48 * 1024 * 1024),
    )(place, gathered, text_raw)


def stages_of(count):
    bits = count.bit_length() - 1
    stages = []
    low = bits
    while low > 1:
        take = 2 if low > 2 else 1
        low -= take
        stages.append((low, take))
    if bits > 0:
        stages.append((0, 1))
    return stages


def gather(shard, count):
    me = lax.axis_index("dp")
    if count & (count - 1):
        return lax.all_gather(shard, "dp", axis=0, tiled=True), me
    place = jnp.zeros((), jnp.int32)
    held = shard
    weight = 1
    for low, take in stages_of(count):
        size = 1 << take
        digit = (me >> low) & (size - 1)
        block = held.shape[0]
        pieces = [held]
        for step in range(1, size):
            pairs = [(i, i ^ (step << low)) for i in range(count)]
            pieces.append(lax.ppermute(held, "dp", pairs))
        joined = jnp.zeros((size * block,) + held.shape[1:], held.dtype)
        for step, piece in enumerate(pieces):
            joined = lax.dynamic_update_slice_in_dim(joined, piece, (digit ^ step) * block, 0)
        held = joined
        place = place + digit * weight
        weight *= size
    return held, place


def local(count, features, ln_gain, w_query, w_key, w_value, w_out, text_raw):
    images, tokens, width = features.shape
    total = images * count
    shard = embed_call(features, ln_gain, w_query, w_key, w_value, w_out, text_raw)
    gathered, place = gather(shard, count)
    if total <= 512:
        loss, text_grad, w_out_grad = contrast_call(place.reshape(1), gathered, text_raw)
    else:
        txt = gathered[:, 0:width]
        img = gathered[:, width : 2 * width]
        abn = gathered[:, 2 * width :]
        loss, delta, w_out_grad = contrast(txt, img, abn)
        own = lax.dynamic_slice_in_dim(delta, place * images, images, 1)
        text_grad = text_back(text_raw, inv_temp * fdot(own, img, ((0,), (0,))))
    return loss.reshape(()), text_grad, w_out_grad


def solution(mesh):
    placed = (P("dp", None, None), P(), P(), P(), P(), P(), P("dp", None))
    return jax.shard_map(
        functools.partial(local, mesh.shape["dp"]),
        mesh=mesh,
        in_specs=placed,
        out_specs=(P(), P("dp", None), P()),
        check_vma=False,
    )
```

```python
import functools

import jax
import jax.numpy as jnp
from jax import lax
from jax.experimental import pallas as pl
from jax.experimental.pallas import tpu as pltpu
from jax.sharding import PartitionSpec as P

HEADS = 16
LANES = 128
GROUP = 256

inv_temp = 1.0 / 0.07
attn_temp = 8.0
epsilon = 1e-06
log2e = 1.4426950408889634


def fdot(a, b, dims):
    return lax.dot_general(a, b, (dims, ((), ())), preferred_element_type=jnp.float32)


def split_bf16(x):
    hi = x.astype(jnp.bfloat16)
    lo = (x - hi.astype(jnp.float32)).astype(jnp.bfloat16)
    return hi, lo


def embed_kernel(
    feat_hbm,
    gain_hbm,
    wq_hbm,
    wk_hbm,
    wv_hbm,
    wo_hbm,
    text_hbm,
    out_ref,
    feat,
    gain_ref,
    text_ref,
    wq,
    wk,
    wv,
    wo,
    normed,
    qn,
    kn,
    raw,
    squared,
    expos,
    scale,
    pooled,
    pn_hi,
    pn_lo,
    xbar,
    feat_sem,
    wqk_sem,
    wvo_sem,
):
    images, tokens, width = feat.shape
    groups = width // GROUP
    head = width // HEADS
    half = images * tokens // 2
    chunk = 16

    feat_copy = [
        pltpu.make_async_copy(feat_hbm.at[b], feat.at[b], feat_sem.at[b]) for b in range(images)
    ]
    wq_copy, wk_copy = [], []
    for g in range(groups):
        cols = pl.ds(g * GROUP, GROUP)
        wq_copy.append(pltpu.make_async_copy(wq_hbm.at[:, cols], wq.at[:, cols], wqk_sem.at[2 * g]))
        wk_copy.append(
            pltpu.make_async_copy(wk_hbm.at[:, cols], wk.at[:, cols], wqk_sem.at[2 * g + 1])
        )
    wv_copy = pltpu.make_async_copy(wv_hbm, wv, wvo_sem.at[0])
    wo_copy = pltpu.make_async_copy(wo_hbm, wo, wvo_sem.at[1])
    gain_copy = pltpu.make_async_copy(gain_hbm, gain_ref, wvo_sem.at[2])
    text_copy = pltpu.make_async_copy(text_hbm, text_ref, wvo_sem.at[3])
    gain_copy.start()
    for b in range(images):
        feat_copy[b].start()
    wq_copy[0].start()
    wk_copy[0].start()
    wq_copy[1].start()

    same_head = lax.broadcasted_iota(jnp.int32, (GROUP, GROUP), 0) // head == (
        lax.broadcasted_iota(jnp.int32, (GROUP, GROUP), 1) // head
    )
    block_ones = jnp.where(same_head, 1.0, 0.0).astype(jnp.bfloat16)
    side = lax.rem(lax.broadcasted_iota(jnp.int32, (1, GROUP), 1), LANES) < head
    left = jnp.where(side, 1.0, 0.0).astype(jnp.bfloat16)
    right = jnp.where(side, 0.0, 1.0).astype(jnp.bfloat16)
    share = jnp.where(
        lax.broadcasted_iota(jnp.int32, (1, tokens), 1) == 0, 1.0, 1.0 / (tokens - 1)
    )

    gain_copy.wait()
    gain = gain_ref[...]

    def normalize(b):
        total = None
        for r in range(0, tokens, chunk):
            x = feat[b, r : r + chunk, :].astype(jnp.float32)
            part = x[0:8, :]
            for i in range(8, chunk, 8):
                part = part + x[i : i + 8, :]
            total = part if total is None else total + part
            center = x - jnp.mean(x, axis=-1, keepdims=True)
            spread = jnp.mean(center * center, axis=-1, keepdims=True)
            normed[b * tokens + r : b * tokens + r + chunk, :] = (
                center * lax.rsqrt(spread + epsilon) * gain
            ).astype(jnp.bfloat16)
        first = feat[b, 0:1, :].astype(jnp.float32)
        total = jnp.sum(total, axis=0, keepdims=True)
        xbar[b : b + 1, :] = first + (total - first) * (1.0 / (tokens - 1))

    sub = lax.broadcasted_iota(jnp.int32, (8, tokens), 0)
    tiles = GROUP // LANES
    steps = 4 * groups

    def project(k):
        g, part = k // 4, (k % 4) // 2
        w = wq if k % 2 == 0 else wk
        proj = fdot(
            normed[part * half : (part + 1) * half, :],
            w[:, g * GROUP : (g + 1) * GROUP],
            ((1,), (0,)),
        )
        raw[k % 2] = proj
        squared[k % 2] = (proj * proj).astype(jnp.bfloat16)

    def unit(k):
        g, part = k // 4, (k % 4) // 2
        here = slice(part * half, (part + 1) * half)
        squares = fdot(squared[k % 2], block_ones, ((1,), (0,)))
        out = (raw[k % 2] * lax.rsqrt(squares + epsilon)).astype(jnp.bfloat16)
        if k % 2 == 0:
            qn[g % 2, here, :] = out
        else:
            kn[g % 2, 0, here, :] = out * left
            kn[g % 2, 1, here, :] = out * right

    def members(j):
        quarter = images // 4
        for n in range(quarter * tiles):
            yield n, (j % 4) * quarter + n // tiles, n % tiles

    def score(j):
        g = j // 4
        for n, b, t in members(j):
            here = slice(b * tokens, (b + 1) * tokens)
            cols = slice(t * LANES, (t + 1) * LANES)
            stacked = jnp.concatenate([kn[g % 2, 0, here, cols], kn[g % 2, 1, here, cols]], axis=0)
            scores = fdot(stacked, qn[g % 2, here, cols], ((1,), (1,)))
            expo = jnp.exp2(scores * (attn_temp * log2e))
            first = share / jnp.sum(expo[0:tokens, :], axis=0, keepdims=True)
            second = share / jnp.sum(expo[tokens:, :], axis=0, keepdims=True)
            hi, lo = split_bf16(jnp.where(sub == 0, first, jnp.where(sub == 1, second, 0.0)))
            scale[j % 2, n] = jnp.concatenate([hi, lo], axis=0)
            expos[j % 2, n] = expo.astype(jnp.bfloat16)

    def pool(j):
        for n, b, t in members(j):
            mass = fdot(scale[j % 2, n], expos[j % 2, n], ((1,), (1,)))
            mass = mass[0:8, :] + mass[8:16, :]
            h = 2 * ((j // 4) * tiles + t)
            pooled[b, h : h + 1, :] = mass[0:1, 0:tokens]
            pooled[b, h + 1 : h + 2, :] = mass[1:2, tokens:]

    def spread_keys(b):
        hi, lo = split_bf16(pooled[b])
        both = jnp.concatenate([hi, lo], axis=0)
        pn = fdot(both, normed[b * tokens : (b + 1) * tokens, :], ((1,), (0,)))
        hi, lo = split_bf16(pn[0:HEADS, :] + pn[HEADS : 2 * HEADS, :])
        pn_hi[b * HEADS : (b + 1) * HEADS, :] = hi
        pn_lo[b * HEADS : (b + 1) * HEADS, :] = lo

    for b in range(images // 2):
        feat_copy[b].wait()
    wk_copy[1].start()
    for c in (wq_copy[2], wk_copy[2], wq_copy[3], wk_copy[3], wv_copy, wo_copy, text_copy):
        c.start()
    for b in range(images // 2):
        normalize(b)
    for b in range(images // 2, images):
        feat_copy[b].wait()
    wq_copy[0].wait()
    wk_copy[0].wait()
    for k in range(steps + 6):
        if k == 3:
            for g in range(1, groups):
                wq_copy[g].wait()
                wk_copy[g].wait()
        if k < steps:
            project(k)
        if k < 2:
            normalize(images // 2 + 2 * k)
            normalize(images // 2 + 2 * k + 1)
        if 3 <= k < steps + 3:
            score(k - 3)
        if 1 <= k <= steps:
            unit(k - 1)
        if 4 <= k < steps + 4:
            pool(k - 4)
        if k >= steps + 1:
            quarter = images // 4
            for n in range(quarter):
                if k - steps - 1 < 4:
                    spread_keys((k - steps - 1) * quarter + n)

    text_copy.wait()
    text32 = text_ref[...].astype(jnp.float32)
    txt_norm = jnp.sqrt(jnp.sum(text32 * text32, axis=1, keepdims=True) + epsilon)
    out_ref[:, 0:width] = (text32 / txt_norm).astype(jnp.bfloat16)

    wv_copy.wait()
    full = fdot(pn_hi[...], wv[...], ((1,), (0,))) + fdot(pn_lo[...], wv[...], ((1,), (0,)))
    full = full.reshape(images, HEADS, width)
    h_id = lax.broadcasted_iota(jnp.int32, (images, HEADS, width), 1)
    l_id = lax.broadcasted_iota(jnp.int32, (images, HEADS, width), 2) // head
    abar = jnp.sum(jnp.where(h_id == l_id, full, 0.0), axis=1).astype(jnp.bfloat16)

    wo_copy.wait()
    emb = xbar[...] + fdot(abar, wo[...], ((1,), (0,)))
    emb_norm = jnp.sqrt(jnp.sum(emb * emb, axis=1, keepdims=True) + epsilon)
    out_ref[:, width : 2 * width] = (emb / emb_norm).astype(jnp.bfloat16)
    out_ref[:, 2 * width : 3 * width] = (abar.astype(jnp.float32) / emb_norm).astype(jnp.bfloat16)


def embed_call(features, ln_gain, w_query, w_key, w_value, w_out, text_raw):
    images, tokens, width = features.shape
    rows = images * tokens
    hbm = pl.BlockSpec(memory_space=pltpu.HBM)
    vmem = pl.BlockSpec(memory_space=pltpu.VMEM)
    weight = pltpu.VMEM((width, width), jnp.bfloat16)
    tall = pltpu.VMEM((rows, width), jnp.bfloat16)
    return pl.pallas_call(
        embed_kernel,
        name="embed",
        out_shape=pltpu.VMEM((images, 3 * width), jnp.bfloat16),
        in_specs=[hbm] * 7,
        out_specs=vmem,
        scratch_shapes=[
            pltpu.VMEM((images, tokens, width), jnp.bfloat16),
            pltpu.VMEM((1, width), jnp.float32),
            pltpu.VMEM((images, width), jnp.bfloat16),
            weight,
            weight,
            weight,
            weight,
            tall,
            pltpu.VMEM((2, rows, GROUP), jnp.bfloat16),
            pltpu.VMEM((2, 2, rows, GROUP), jnp.bfloat16),
            pltpu.VMEM((2, rows // 2, GROUP), jnp.float32),
            pltpu.VMEM((2, rows // 2, GROUP), jnp.bfloat16),
            pltpu.VMEM((2, images // 4 * GROUP // LANES, 2 * tokens, tokens), jnp.bfloat16),
            pltpu.VMEM((2, images // 4 * GROUP // LANES, 16, tokens), jnp.bfloat16),
            pltpu.VMEM((images, HEADS, tokens), jnp.float32),
            pltpu.VMEM((images * HEADS, width), jnp.bfloat16),
            pltpu.VMEM((images * HEADS, width), jnp.bfloat16),
            pltpu.VMEM((images, width), jnp.float32),
            pltpu.SemaphoreType.DMA((images,)),
            pltpu.SemaphoreType.DMA((2 * width // GROUP,)),
            pltpu.SemaphoreType.DMA((4,)),
        ],
        compiler_params=pltpu.CompilerParams(vmem_limit_bytes=60 * 1024 * 1024),
    )(features, ln_gain.reshape(1, width), w_query, w_key, w_value, w_out, text_raw)


def weigh(logits):
    total = logits.shape[0]
    row_id = lax.broadcasted_iota(jnp.int32, (total, total), 0)
    col_id = lax.broadcasted_iota(jnp.int32, (total, total), 1)
    eye = row_id == col_id
    expo = jnp.exp(logits)
    rowsum = jnp.sum(expo, axis=1, keepdims=True)
    colsum = jnp.sum(expo, axis=0, keepdims=True)
    diag = jnp.sum(jnp.where(eye, logits, 0.0), axis=1, keepdims=True)
    loss = (
        jnp.sum(jnp.log(rowsum) - 2.0 * diag, axis=0, keepdims=True)
        + jnp.sum(jnp.log(colsum), axis=1, keepdims=True)
    ) / (2.0 * total)
    delta = expo * (0.5 / rowsum) + expo * (0.5 / colsum) - jnp.where(eye, 1.0, 0.0)
    return loss, delta.astype(jnp.bfloat16)


def raw_emb_grad(delta, txt, img):
    grad_img = inv_temp * fdot(delta, txt, ((1,), (0,)))
    img32 = img.astype(jnp.float32)
    along = jnp.sum(img32 * grad_img, axis=1, keepdims=True)
    return split_bf16(grad_img - img32 * along)


def text_back(text_raw, grad_txt):
    text32 = text_raw.astype(jnp.float32)
    txt_norm = jnp.sqrt(jnp.sum(text32 * text32, axis=1, keepdims=True) + epsilon)
    txt_f = text32 / txt_norm
    return (grad_txt - txt_f * jnp.sum(txt_f * grad_txt, axis=1, keepdims=True)) / txt_norm


def contrast_kernel(
    place_ref, all_ref, text_hbm, loss_ref, text_grad_ref, w_grad_hbm, text, delta_t, w_grad, sem
):
    images, width = text.shape
    blocks = width // GROUP
    text_copy = pltpu.make_async_copy(text_hbm, text, sem.at[blocks])
    text_copy.start()
    txt = all_ref[:, 0:width]
    img = all_ref[:, width : 2 * width]
    loss, delta = weigh(inv_temp * fdot(img, txt, ((1,), (1,))))
    loss_ref[...] = loss
    hi, lo = raw_emb_grad(delta, txt, img)
    copies = []
    for i in range(blocks):
        cols = slice(i * GROUP, (i + 1) * GROUP)
        abn = all_ref[:, 2 * width + i * GROUP : 2 * width + (i + 1) * GROUP]
        part = fdot(abn, hi, ((0,), (0,))) + fdot(abn, lo, ((0,), (0,)))
        w_grad[cols, :] = part.astype(jnp.bfloat16)
        copies.append(pltpu.make_async_copy(w_grad.at[cols], w_grad_hbm.at[cols], sem.at[i]))
        copies[-1].start()
    delta_t[...] = jnp.transpose(delta.astype(jnp.float32))
    own = delta_t[pl.ds(pl.multiple_of(place_ref[0] * images, images), images), :]
    grad_txt = inv_temp * fdot(own.astype(jnp.bfloat16), img, ((1,), (0,)))
    text_copy.wait()
    text_grad_ref[...] = text_back(text[...], grad_txt)
    for c in copies:
        c.wait()


def contrast_call(place, gathered, text_raw):
    total = gathered.shape[0]
    images, width = text_raw.shape
    vmem = pl.BlockSpec(memory_space=pltpu.VMEM)
    hbm = pl.BlockSpec(memory_space=pltpu.HBM)
    return pl.pallas_call(
        contrast_kernel,
        name="contrast",
        out_shape=(
            jax.ShapeDtypeStruct((1, 1), jnp.float32),
            jax.ShapeDtypeStruct((images, width), jnp.float32),
            jax.ShapeDtypeStruct((width, width), jnp.bfloat16),
        ),
        in_specs=[pl.BlockSpec(memory_space=pltpu.SMEM), vmem, hbm],
        out_specs=(vmem, vmem, hbm),
        scratch_shapes=[
            pltpu.VMEM((images, width), jnp.bfloat16),
            pltpu.VMEM((total, total), jnp.float32),
            pltpu.VMEM((width, width), jnp.bfloat16),
            pltpu.SemaphoreType.DMA((width // GROUP + 1,)),
        ],
        compiler_params=pltpu.CompilerParams(vmem_limit_bytes=48 * 1024 * 1024),
    )(place, gathered, text_raw)


def stages_of(count):
    bits = count.bit_length() - 1
    stages = []
    low = bits
    while low > 1:
        take = 2 if low > 2 else 1
        low -= take
        stages.append((low, take))
    if bits > 0:
        stages.append((0, 1))
    return stages


def gather(shard, count):
    me = lax.axis_index("dp")
    if count & (count - 1):
        return lax.all_gather(shard, "dp", axis=0, tiled=True), me
    place = jnp.zeros((), jnp.int32)
    held = shard
    weight = 1
    for low, take in stages_of(count):
        size = 1 << take
        digit = (me >> low) & (size - 1)
        block = held.shape[0]
        pieces = [held]
        for step in range(1, size):
            pairs = [(i, i ^ (step << low)) for i in range(count)]
            pieces.append(lax.ppermute(held, "dp", pairs))
        joined = jnp.zeros((size * block,) + held.shape[1:], held.dtype)
        for step, piece in enumerate(pieces):
            joined = lax.dynamic_update_slice_in_dim(joined, piece, (digit ^ step) * block, 0)
        held = joined
        place = place + digit * weight
        weight *= size
    return held, place


def local(count, features, ln_gain, w_query, w_key, w_value, w_out, text_raw):
    images, tokens, width = features.shape
    total = images * count
    shard = embed_call(features, ln_gain, w_query, w_key, w_value, w_out, text_raw)
    gathered, place = gather(shard, count)
    if total <= 512:
        loss, text_grad, w_out_grad = contrast_call(place.reshape(1), gathered, text_raw)
    else:
        txt = gathered[:, 0:width]
        img = gathered[:, width : 2 * width]
        abn = gathered[:, 2 * width :]
        loss, delta = weigh(inv_temp * fdot(img, txt, ((1,), (1,))))
        hi, lo = raw_emb_grad(delta, txt, img)
        w_out_grad = fdot(abn, hi, ((0,), (0,))) + fdot(abn, lo, ((0,), (0,)))
        w_out_grad = w_out_grad.astype(jnp.bfloat16)
        own = lax.dynamic_slice_in_dim(delta, place * images, images, 1)
        text_grad = text_back(text_raw, inv_temp * fdot(own, img, ((0,), (0,))))
    return loss.reshape(()), text_grad, w_out_grad


def solution(mesh):
    placed = (P("dp", None, None), P(), P(), P(), P(), P(), P("dp", None))
    return jax.shard_map(
        functools.partial(local, mesh.shape["dp"]),
        mesh=mesh,
        in_specs=placed,
        out_specs=(P(), P("dp", None), P()),
        check_vma=False,
    )
```

```python
import functools

import jax
import jax.numpy as jnp
from jax import lax
from jax.experimental import pallas as pl
from jax.experimental.pallas import tpu as pltpu
from jax.sharding import PartitionSpec as P

HEADS = 16
LANES = 128
GROUP = 256

inv_temp = 1.0 / 0.07
attn_temp = 8.0
epsilon = 1e-06
log2e = 1.4426950408889634


def fdot(a, b, dims):
    return lax.dot_general(a, b, (dims, ((), ())), preferred_element_type=jnp.float32)


def split_bf16(x):
    hi = x.astype(jnp.bfloat16)
    lo = (x - hi.astype(jnp.float32)).astype(jnp.bfloat16)
    return hi, lo


def embed_kernel(
    feat_hbm,
    gain_hbm,
    wq_hbm,
    wk_hbm,
    wv_hbm,
    wo_hbm,
    text_hbm,
    out_ref,
    feat,
    gain_ref,
    text_ref,
    wq,
    wk,
    wv,
    wo,
    normed,
    qn,
    kn,
    raw,
    squared,
    expos,
    scale,
    pooled,
    pn_hi,
    pn_lo,
    xbar,
    feat_sem,
    wqk_sem,
    wvo_sem,
):
    images, tokens, width = feat.shape
    groups = width // GROUP
    head = width // HEADS
    half = images * tokens // 2
    chunk = 16

    feat_copy = [
        pltpu.make_async_copy(feat_hbm.at[b], feat.at[b], feat_sem.at[b]) for b in range(images)
    ]
    wq_copy, wk_copy = [], []
    for g in range(groups):
        cols = pl.ds(g * GROUP, GROUP)
        wq_copy.append(pltpu.make_async_copy(wq_hbm.at[:, cols], wq.at[:, cols], wqk_sem.at[2 * g]))
        wk_copy.append(
            pltpu.make_async_copy(wk_hbm.at[:, cols], wk.at[:, cols], wqk_sem.at[2 * g + 1])
        )
    wv_copy = pltpu.make_async_copy(wv_hbm, wv, wvo_sem.at[0])
    wo_copy = pltpu.make_async_copy(wo_hbm, wo, wvo_sem.at[1])
    gain_copy = pltpu.make_async_copy(gain_hbm, gain_ref, wvo_sem.at[2])
    text_copy = pltpu.make_async_copy(text_hbm, text_ref, wvo_sem.at[3])
    gain_copy.start()
    for b in range(images // 2):
        feat_copy[b].start()
    wq_copy[0].start()

    same_head = lax.broadcasted_iota(jnp.int32, (GROUP, GROUP), 0) // head == (
        lax.broadcasted_iota(jnp.int32, (GROUP, GROUP), 1) // head
    )
    block_ones = jnp.where(same_head, 1.0, 0.0).astype(jnp.bfloat16)
    side = lax.rem(lax.broadcasted_iota(jnp.int32, (1, GROUP), 1), LANES) < head
    left = jnp.where(side, 1.0, 0.0).astype(jnp.bfloat16)
    right = jnp.where(side, 0.0, 1.0).astype(jnp.bfloat16)
    share = jnp.where(
        lax.broadcasted_iota(jnp.int32, (1, tokens), 1) == 0, 1.0, 1.0 / (tokens - 1)
    )

    gain_copy.wait()
    gain = gain_ref[...]

    def normalize(b):
        total = None
        for r in range(0, tokens, chunk):
            x = feat[b, r : r + chunk, :].astype(jnp.float32)
            part = x[0:8, :]
            for i in range(8, chunk, 8):
                part = part + x[i : i + 8, :]
            total = part if total is None else total + part
            center = x - jnp.mean(x, axis=-1, keepdims=True)
            spread = jnp.mean(center * center, axis=-1, keepdims=True)
            normed[b * tokens + r : b * tokens + r + chunk, :] = (
                center * lax.rsqrt(spread + epsilon) * gain
            ).astype(jnp.bfloat16)
        first = feat[b, 0:1, :].astype(jnp.float32)
        total = jnp.sum(total, axis=0, keepdims=True)
        xbar[b : b + 1, :] = first + (total - first) * (1.0 / (tokens - 1))

    sub = lax.broadcasted_iota(jnp.int32, (8, tokens), 0)
    tiles = GROUP // LANES
    steps = 4 * groups

    def project(k):
        g, part = k // 4, (k % 4) // 2
        w = wq if k % 2 == 0 else wk
        proj = fdot(
            normed[part * half : (part + 1) * half, :],
            w[:, g * GROUP : (g + 1) * GROUP],
            ((1,), (0,)),
        )
        raw[k % 2] = proj
        squared[k % 2] = (proj * proj).astype(jnp.bfloat16)

    def unit(k):
        g, part = k // 4, (k % 4) // 2
        here = slice(part * half, (part + 1) * half)
        squares = fdot(squared[k % 2], block_ones, ((1,), (0,)))
        out = (raw[k % 2] * lax.rsqrt(squares + epsilon)).astype(jnp.bfloat16)
        if k % 2 == 0:
            qn[g % 2, here, :] = out
        else:
            kn[g % 2, 0, here, :] = out * left
            kn[g % 2, 1, here, :] = out * right

    def members(j):
        quarter = images // 4
        for n in range(quarter * tiles):
            yield n, (j % 4) * quarter + n // tiles, n % tiles

    def score(j):
        g = j // 4
        for n, b, t in members(j):
            here = slice(b * tokens, (b + 1) * tokens)
            cols = slice(t * LANES, (t + 1) * LANES)
            stacked = jnp.concatenate([kn[g % 2, 0, here, cols], kn[g % 2, 1, here, cols]], axis=0)
            scores = fdot(stacked, qn[g % 2, here, cols], ((1,), (1,)))
            expo = jnp.exp2(scores * (attn_temp * log2e))
            first = share / jnp.sum(expo[0:tokens, :], axis=0, keepdims=True)
            second = share / jnp.sum(expo[tokens:, :], axis=0, keepdims=True)
            hi, lo = split_bf16(jnp.where(sub == 0, first, jnp.where(sub == 1, second, 0.0)))
            scale[j % 2, n] = jnp.concatenate([hi, lo], axis=0)
            expos[j % 2, n] = expo.astype(jnp.bfloat16)

    def pool(j):
        for n, b, t in members(j):
            mass = fdot(scale[j % 2, n], expos[j % 2, n], ((1,), (1,)))
            mass = mass[0:8, :] + mass[8:16, :]
            h = 2 * ((j // 4) * tiles + t)
            pooled[b, h : h + 1, :] = mass[0:1, 0:tokens]
            pooled[b, h + 1 : h + 2, :] = mass[1:2, tokens:]

    def spread_keys(b):
        hi, lo = split_bf16(pooled[b])
        both = jnp.concatenate([hi, lo], axis=0)
        pn = fdot(both, normed[b * tokens : (b + 1) * tokens, :], ((1,), (0,)))
        hi, lo = split_bf16(pn[0:HEADS, :] + pn[HEADS : 2 * HEADS, :])
        pn_hi[b * HEADS : (b + 1) * HEADS, :] = hi
        pn_lo[b * HEADS : (b + 1) * HEADS, :] = lo

    for b in range(images // 2):
        feat_copy[b].wait()
    wk_copy[0].start()
    for b in range(images // 2, images):
        feat_copy[b].start()
    for b in range(images // 4):
        normalize(b)
    wq_copy[1].start()
    wk_copy[1].start()
    for b in range(images // 4, images // 2):
        normalize(b)
    wq_copy[0].wait()
    wk_copy[0].wait()
    for b in range(images // 2, images):
        feat_copy[b].wait()
    for k in range(steps + 6):
        if k < 2:
            wq_copy[k + 2].start()
            wk_copy[k + 2].start()
        if k == 4:
            text_copy.start()
            wv_copy.start()
        if k == 6:
            wo_copy.start()
        if k == 3:
            wq_copy[1].wait()
            wk_copy[1].wait()
        if k == 6:
            for g in range(2, groups):
                wq_copy[g].wait()
                wk_copy[g].wait()
        if k < steps:
            project(k)
        if k < 2:
            normalize(images // 2 + 2 * k)
            normalize(images // 2 + 2 * k + 1)
        if 3 <= k < steps + 3:
            score(k - 3)
        if 1 <= k <= steps:
            unit(k - 1)
        if 4 <= k < steps + 4:
            pool(k - 4)
        if k >= steps + 1:
            quarter = images // 4
            for n in range(quarter):
                if k - steps - 1 < 4:
                    spread_keys((k - steps - 1) * quarter + n)

    text_copy.wait()
    text32 = text_ref[...].astype(jnp.float32)
    txt_norm = jnp.sqrt(jnp.sum(text32 * text32, axis=1, keepdims=True) + epsilon)
    out_ref[:, 0:width] = (text32 / txt_norm).astype(jnp.bfloat16)

    wv_copy.wait()
    full = fdot(pn_hi[...], wv[...], ((1,), (0,))) + fdot(pn_lo[...], wv[...], ((1,), (0,)))
    full = full.reshape(images, HEADS, width)
    h_id = lax.broadcasted_iota(jnp.int32, (images, HEADS, width), 1)
    l_id = lax.broadcasted_iota(jnp.int32, (images, HEADS, width), 2) // head
    abar = jnp.sum(jnp.where(h_id == l_id, full, 0.0), axis=1).astype(jnp.bfloat16)

    wo_copy.wait()
    emb = xbar[...] + fdot(abar, wo[...], ((1,), (0,)))
    emb_norm = jnp.sqrt(jnp.sum(emb * emb, axis=1, keepdims=True) + epsilon)
    out_ref[:, width : 2 * width] = (emb / emb_norm).astype(jnp.bfloat16)
    out_ref[:, 2 * width : 3 * width] = (abar.astype(jnp.float32) / emb_norm).astype(jnp.bfloat16)


def embed_call(features, ln_gain, w_query, w_key, w_value, w_out, text_raw):
    images, tokens, width = features.shape
    rows = images * tokens
    hbm = pl.BlockSpec(memory_space=pltpu.HBM)
    vmem = pl.BlockSpec(memory_space=pltpu.VMEM)
    weight = pltpu.VMEM((width, width), jnp.bfloat16)
    tall = pltpu.VMEM((rows, width), jnp.bfloat16)
    return pl.pallas_call(
        embed_kernel,
        name="embed",
        out_shape=pltpu.VMEM((images, 3 * width), jnp.bfloat16),
        in_specs=[hbm] * 7,
        out_specs=vmem,
        scratch_shapes=[
            pltpu.VMEM((images, tokens, width), jnp.bfloat16),
            pltpu.VMEM((1, width), jnp.float32),
            pltpu.VMEM((images, width), jnp.bfloat16),
            weight,
            weight,
            weight,
            weight,
            tall,
            pltpu.VMEM((2, rows, GROUP), jnp.bfloat16),
            pltpu.VMEM((2, 2, rows, GROUP), jnp.bfloat16),
            pltpu.VMEM((2, rows // 2, GROUP), jnp.float32),
            pltpu.VMEM((2, rows // 2, GROUP), jnp.bfloat16),
            pltpu.VMEM((2, images // 4 * GROUP // LANES, 2 * tokens, tokens), jnp.bfloat16),
            pltpu.VMEM((2, images // 4 * GROUP // LANES, 16, tokens), jnp.bfloat16),
            pltpu.VMEM((images, HEADS, tokens), jnp.float32),
            pltpu.VMEM((images * HEADS, width), jnp.bfloat16),
            pltpu.VMEM((images * HEADS, width), jnp.bfloat16),
            pltpu.VMEM((images, width), jnp.float32),
            pltpu.SemaphoreType.DMA((images,)),
            pltpu.SemaphoreType.DMA((2 * width // GROUP,)),
            pltpu.SemaphoreType.DMA((4,)),
        ],
        compiler_params=pltpu.CompilerParams(vmem_limit_bytes=60 * 1024 * 1024),
    )(features, ln_gain.reshape(1, width), w_query, w_key, w_value, w_out, text_raw)


def weigh(logits):
    total = logits.shape[0]
    row_id = lax.broadcasted_iota(jnp.int32, (total, total), 0)
    col_id = lax.broadcasted_iota(jnp.int32, (total, total), 1)
    eye = row_id == col_id
    expo = jnp.exp(logits)
    rowsum = jnp.sum(expo, axis=1, keepdims=True)
    colsum = jnp.sum(expo, axis=0, keepdims=True)
    diag = jnp.sum(jnp.where(eye, logits, 0.0), axis=1, keepdims=True)
    loss = (
        jnp.sum(jnp.log(rowsum) - 2.0 * diag, axis=0, keepdims=True)
        + jnp.sum(jnp.log(colsum), axis=1, keepdims=True)
    ) / (2.0 * total)
    delta = expo * (0.5 / rowsum) + expo * (0.5 / colsum) - jnp.where(eye, 1.0, 0.0)
    return loss, delta.astype(jnp.bfloat16)


def raw_emb_grad(delta, txt, img):
    grad_img = inv_temp * fdot(delta, txt, ((1,), (0,)))
    img32 = img.astype(jnp.float32)
    along = jnp.sum(img32 * grad_img, axis=1, keepdims=True)
    return (grad_img - img32 * along).astype(jnp.bfloat16)


def text_back(text_raw, grad_txt):
    text32 = text_raw.astype(jnp.float32)
    txt_norm = jnp.sqrt(jnp.sum(text32 * text32, axis=1, keepdims=True) + epsilon)
    txt_f = text32 / txt_norm
    return (grad_txt - txt_f * jnp.sum(txt_f * grad_txt, axis=1, keepdims=True)) / txt_norm


def contrast_kernel(
    place_ref,
    all_ref,
    text_hbm,
    loss_hbm,
    text_grad_hbm,
    w_grad_hbm,
    text,
    delta_t,
    loss_out,
    text_grad,
    w_grad,
    sem,
):
    images, width = text.shape
    blocks = width // GROUP
    text_copy = pltpu.make_async_copy(text_hbm, text, sem.at[blocks])
    text_copy.start()
    txt = all_ref[:, 0:width]
    img = all_ref[:, width : 2 * width]
    loss, delta = weigh(inv_temp * fdot(img, txt, ((1,), (1,))))
    loss_out[...] = loss
    copies = [pltpu.make_async_copy(loss_out, loss_hbm, sem.at[blocks + 1])]
    copies[0].start()
    delta_t[...] = jnp.transpose(delta.astype(jnp.float32))
    emb_grad = raw_emb_grad(delta, txt, img)
    own = delta_t[pl.ds(pl.multiple_of(place_ref[0] * images, images), images), :]
    grad_txt = inv_temp * fdot(own.astype(jnp.bfloat16), img, ((1,), (0,)))
    text_copy.wait()
    text_grad[...] = text_back(text[...], grad_txt)
    copies.append(pltpu.make_async_copy(text_grad, text_grad_hbm, sem.at[blocks + 2]))
    copies[1].start()
    for i in range(blocks):
        cols = slice(i * GROUP, (i + 1) * GROUP)
        abn = all_ref[:, 2 * width + i * GROUP : 2 * width + (i + 1) * GROUP]
        w_grad[cols, :] = fdot(abn, emb_grad, ((0,), (0,))).astype(jnp.bfloat16)
        copies.append(pltpu.make_async_copy(w_grad.at[cols], w_grad_hbm.at[cols], sem.at[i]))
        copies[-1].start()
    for c in copies:
        c.wait()


def contrast_call(place, gathered, text_raw):
    total = gathered.shape[0]
    images, width = text_raw.shape
    vmem = pl.BlockSpec(memory_space=pltpu.VMEM)
    hbm = pl.BlockSpec(memory_space=pltpu.HBM)
    return pl.pallas_call(
        contrast_kernel,
        name="contrast",
        out_shape=(
            jax.ShapeDtypeStruct((1, 1), jnp.float32),
            jax.ShapeDtypeStruct((images, width), jnp.float32),
            jax.ShapeDtypeStruct((width, width), jnp.bfloat16),
        ),
        in_specs=[pl.BlockSpec(memory_space=pltpu.SMEM), vmem, hbm],
        out_specs=(hbm, hbm, hbm),
        scratch_shapes=[
            pltpu.VMEM((images, width), jnp.bfloat16),
            pltpu.VMEM((total, total), jnp.float32),
            pltpu.VMEM((1, 1), jnp.float32),
            pltpu.VMEM((images, width), jnp.float32),
            pltpu.VMEM((width, width), jnp.bfloat16),
            pltpu.SemaphoreType.DMA((width // GROUP + 3,)),
        ],
        compiler_params=pltpu.CompilerParams(vmem_limit_bytes=48 * 1024 * 1024),
    )(place, gathered, text_raw)


def stages_of(count):
    bits = count.bit_length() - 1
    stages = []
    low = bits
    while low > 1:
        take = 2 if low > 2 else 1
        low -= take
        stages.append((low, take))
    if bits > 0:
        stages.append((0, 1))
    return stages


def gather(shard, count):
    me = lax.axis_index("dp")
    if count & (count - 1):
        return lax.all_gather(shard, "dp", axis=0, tiled=True), me
    bits = count.bit_length() - 1
    place = jnp.zeros((), jnp.int32)
    held = shard
    weight = 1
    for low, take in stages_of(count):
        size = 1 << take
        digit = (me >> low) & (size - 1)
        block = held.shape[0]
        pieces = [held]
        order = [2, 3, 1] if low + take == bits else [3, 2, 1]
        order = [step for step in order if step < size]
        for step in order:
            pairs = [(i, i ^ (step << low)) for i in range(count)]
            pieces.append(lax.ppermute(held, "dp", pairs))
        joined = jnp.zeros((size * block,) + held.shape[1:], held.dtype)
        for step, piece in zip([0] + order, pieces):
            joined = lax.dynamic_update_slice_in_dim(joined, piece, (digit ^ step) * block, 0)
        held = joined
        place = place + digit * weight
        weight *= size
    return held, place


def local(count, features, ln_gain, w_query, w_key, w_value, w_out, text_raw):
    images, tokens, width = features.shape
    total = images * count
    shard = embed_call(features, ln_gain, w_query, w_key, w_value, w_out, text_raw)
    gathered, place = gather(shard, count)
    if total <= 512:
        loss, text_grad, w_out_grad = contrast_call(place.reshape(1), gathered, text_raw)
    else:
        txt = gathered[:, 0:width]
        img = gathered[:, width : 2 * width]
        abn = gathered[:, 2 * width :]
        loss, delta = weigh(inv_temp * fdot(img, txt, ((1,), (1,))))
        emb_grad = raw_emb_grad(delta, txt, img)
        w_out_grad = fdot(abn, emb_grad, ((0,), (0,)))
        w_out_grad = w_out_grad.astype(jnp.bfloat16)
        own = lax.dynamic_slice_in_dim(delta, place * images, images, 1)
        text_grad = text_back(text_raw, inv_temp * fdot(own, img, ((0,), (0,))))
    return loss.reshape(()), text_grad, w_out_grad


def solution(mesh):
    placed = (P("dp", None, None), P(), P(), P(), P(), P(), P("dp", None))
    return jax.shard_map(
        functools.partial(local, mesh.shape["dp"]),
        mesh=mesh,
        in_specs=placed,
        out_specs=(P(), P("dp", None), P()),
        check_vma=False,
    )
```

```python
import functools

import jax
import jax.numpy as jnp
from jax import lax
from jax.experimental import pallas as pl
from jax.experimental.pallas import tpu as pltpu
from jax.sharding import PartitionSpec as P

HEADS = 16
LANES = 128
GROUP = 256

inv_temp = 1.0 / 0.07
attn_temp = 8.0
epsilon = 1e-06
log2e = 1.4426950408889634


def fdot(a, b, dims):
    return lax.dot_general(a, b, (dims, ((), ())), preferred_element_type=jnp.float32)


def split_bf16(x):
    hi = x.astype(jnp.bfloat16)
    lo = (x - hi.astype(jnp.float32)).astype(jnp.bfloat16)
    return hi, lo


def embed_kernel(
    feat_hbm,
    gain_hbm,
    wq_hbm,
    wk_hbm,
    wv_hbm,
    wo_hbm,
    text_hbm,
    out_ref,
    feat,
    gain_ref,
    text_ref,
    wq,
    wk,
    wv,
    wo,
    normed,
    qn,
    kn,
    raw,
    squared,
    expos,
    scale,
    pooled,
    pn_hi,
    pn_lo,
    xbar,
    feat_sem,
    wqk_sem,
    wvo_sem,
):
    images, tokens, width = feat.shape
    groups = width // GROUP
    head = width // HEADS
    half = images * tokens // 2
    chunk = 16

    feat_copy = [
        pltpu.make_async_copy(feat_hbm.at[b], feat.at[b], feat_sem.at[b]) for b in range(images)
    ]
    wq_copy, wk_copy = [], []
    for g in range(groups):
        cols = pl.ds(g * GROUP, GROUP)
        wq_copy.append(pltpu.make_async_copy(wq_hbm.at[:, cols], wq.at[:, cols], wqk_sem.at[2 * g]))
        wk_copy.append(
            pltpu.make_async_copy(wk_hbm.at[:, cols], wk.at[:, cols], wqk_sem.at[2 * g + 1])
        )
    wv_copy = pltpu.make_async_copy(wv_hbm, wv, wvo_sem.at[0])
    wo_copy = pltpu.make_async_copy(wo_hbm, wo, wvo_sem.at[1])
    gain_copy = pltpu.make_async_copy(gain_hbm, gain_ref, wvo_sem.at[2])
    text_copy = pltpu.make_async_copy(text_hbm, text_ref, wvo_sem.at[3])
    gain_copy.start()
    for b in range(images // 2):
        feat_copy[b].start()
    wq_copy[0].start()
    wk_copy[0].start()
    for b in range(images // 2, images):
        feat_copy[b].start()

    same_head = lax.broadcasted_iota(jnp.int32, (GROUP, GROUP), 0) // head == (
        lax.broadcasted_iota(jnp.int32, (GROUP, GROUP), 1) // head
    )
    block_ones = jnp.where(same_head, 1.0, 0.0).astype(jnp.bfloat16)
    side = lax.rem(lax.broadcasted_iota(jnp.int32, (1, GROUP), 1), LANES) < head
    left = jnp.where(side, 1.0, 0.0).astype(jnp.bfloat16)
    right = jnp.where(side, 0.0, 1.0).astype(jnp.bfloat16)
    share = jnp.where(
        lax.rem(lax.broadcasted_iota(jnp.int32, (1, 2 * tokens), 1), tokens) == 0,
        1.0,
        1.0 / (tokens - 1),
    )

    gain_copy.wait()
    gain = gain_ref[...]

    def normalize(b):
        total = None
        for r in range(0, tokens, chunk):
            x = feat[b, r : r + chunk, :].astype(jnp.float32)
            part = x[0:8, :]
            for i in range(8, chunk, 8):
                part = part + x[i : i + 8, :]
            total = part if total is None else total + part
            center = x - jnp.mean(x, axis=-1, keepdims=True)
            spread = jnp.mean(center * center, axis=-1, keepdims=True)
            normed[b * tokens + r : b * tokens + r + chunk, :] = (
                center * lax.rsqrt(spread + epsilon) * gain
            ).astype(jnp.bfloat16)
        first = feat[b, 0:1, :].astype(jnp.float32)
        total = jnp.sum(total, axis=0, keepdims=True)
        xbar[b : b + 1, :] = first + (total - first) * (1.0 / (tokens - 1))

    head_lane = lax.broadcasted_iota(jnp.int32, (tokens, LANES), 1)
    tiles = GROUP // LANES
    steps = 4 * groups

    def project(k):
        g, part = k // 4, (k % 4) // 2
        w = wq if k % 2 == 0 else wk
        proj = fdot(
            normed[part * half : (part + 1) * half, :],
            w[:, g * GROUP : (g + 1) * GROUP],
            ((1,), (0,)),
        )
        raw[k % 2] = proj
        squared[k % 2] = (proj * proj).astype(jnp.bfloat16)

    def unit(k):
        g, part = k // 4, (k % 4) // 2
        here = slice(part * half, (part + 1) * half)
        squares = fdot(squared[k % 2], block_ones, ((1,), (0,)))
        out = (raw[k % 2] * lax.rsqrt(squares + epsilon)).astype(jnp.bfloat16)
        if k % 2 == 0:
            qn[g % 2, 0, here, :] = out * left
            qn[g % 2, 1, here, :] = out * right
        else:
            kn[g % 2, here, :] = out

    def members(j):
        quarter = images // 4
        for n in range(quarter * tiles):
            yield n, (j % 4) * quarter + n // tiles, n % tiles

    def score(j):
        g = j // 4
        for n, b, t in members(j):
            here = slice(b * tokens, (b + 1) * tokens)
            cols = slice(t * LANES, (t + 1) * LANES)
            stacked = jnp.concatenate([qn[g % 2, 0, here, cols], qn[g % 2, 1, here, cols]], axis=0)
            scores = fdot(kn[g % 2, here, cols], stacked, ((1,), (1,)))
            expo = jnp.exp2(scores * (attn_temp * log2e))
            inverse = share / jnp.sum(expo, axis=0, keepdims=True)
            scale[j % 2, n] = inverse
            expos[j % 2, n] = expo

    def pool(j):
        for n, b, t in members(j):
            weighted = expos[j % 2, n] * scale[j % 2, n]
            h = 2 * ((j // 4) * tiles + t)
            old = pooled[b] if h else jnp.zeros((tokens, LANES), jnp.float32)
            for i in range(2):
                mass = jnp.sum(weighted[:, i * tokens : (i + 1) * tokens], axis=1, keepdims=True)
                old = jnp.where(head_lane == h + i, mass, old)
            pooled[b] = old

    def spread_keys(b):
        hi, lo = split_bf16(jnp.transpose(pooled[b])[0:HEADS, :])
        both = jnp.concatenate([hi, lo], axis=0)
        pn = fdot(both, normed[b * tokens : (b + 1) * tokens, :], ((1,), (0,)))
        hi, lo = split_bf16(pn[0:HEADS, :] + pn[HEADS : 2 * HEADS, :])
        pn_hi[b * HEADS : (b + 1) * HEADS, :] = hi
        pn_lo[b * HEADS : (b + 1) * HEADS, :] = lo

    for b in range(images // 2):
        feat_copy[b].wait()
    wq_copy[1].start()
    wk_copy[1].start()
    for b in range(images // 2):
        normalize(b)
    wq_copy[0].wait()
    wk_copy[0].wait()
    for b in range(images // 2, images):
        feat_copy[b].wait()
    for k in range(steps + 6):
        if k < 2:
            wq_copy[k + 2].start()
            wk_copy[k + 2].start()
        if k == 1:
            text_copy.start()
            wv_copy.start()
            wo_copy.start()
        if k == 4:
            for g in range(1, groups):
                wq_copy[g].wait()
                wk_copy[g].wait()
        if k == 8:
            text_copy.wait()
            wv_copy.wait()
            wo_copy.wait()
        if k < steps:
            project(k)
        if k < 2:
            normalize(images // 2 + 2 * k)
            normalize(images // 2 + 2 * k + 1)
        if 3 <= k < steps + 3:
            score(k - 3)
        if 1 <= k <= steps:
            unit(k - 1)
        if 4 <= k < steps + 4:
            pool(k - 4)
        if k >= steps + 1:
            quarter = images // 4
            for n in range(quarter):
                if k - steps - 1 < 4:
                    spread_keys((k - steps - 1) * quarter + n)

    text32 = text_ref[...].astype(jnp.float32)
    txt_norm = jnp.sqrt(jnp.sum(text32 * text32, axis=1, keepdims=True) + epsilon)
    out_ref[:, 0:width] = (text32 / txt_norm).astype(jnp.bfloat16)

    h_id = lax.broadcasted_iota(jnp.int32, (images, HEADS, GROUP), 1)
    l_id = lax.broadcasted_iota(jnp.int32, (images, HEADS, GROUP), 2) // head
    abar = []
    emb = xbar[...]
    for g in range(groups + 1):
        cols = slice(g * GROUP, (g + 1) * GROUP)
        if g < groups:
            full = fdot(pn_hi[...], wv[:, cols], ((1,), (0,)))
            full = full + fdot(pn_lo[...], wv[:, cols], ((1,), (0,)))
        if g > 0:
            rows = slice((g - 1) * GROUP, g * GROUP)
            emb = emb + fdot(abar[g - 1], wo[rows, :], ((1,), (0,)))
        if g < groups:
            own = h_id == l_id + g * (GROUP // head)
            full = jnp.where(own, full.reshape(images, HEADS, GROUP), 0.0)
            abar.append(jnp.sum(full, axis=1).astype(jnp.bfloat16))
    abar = jnp.concatenate(abar, axis=1)

    emb_norm = jnp.sqrt(jnp.sum(emb * emb, axis=1, keepdims=True) + epsilon)
    out_ref[:, width : 2 * width] = (emb / emb_norm).astype(jnp.bfloat16)
    out_ref[:, 2 * width : 3 * width] = (abar.astype(jnp.float32) / emb_norm).astype(jnp.bfloat16)


def embed_call(features, ln_gain, w_query, w_key, w_value, w_out, text_raw):
    images, tokens, width = features.shape
    rows = images * tokens
    hbm = pl.BlockSpec(memory_space=pltpu.HBM)
    vmem = pl.BlockSpec(memory_space=pltpu.VMEM)
    weight = pltpu.VMEM((width, width), jnp.bfloat16)
    tall = pltpu.VMEM((rows, width), jnp.bfloat16)
    return pl.pallas_call(
        embed_kernel,
        name="embed",
        out_shape=pltpu.VMEM((images, 3 * width), jnp.bfloat16),
        in_specs=[hbm] * 7,
        out_specs=vmem,
        scratch_shapes=[
            pltpu.VMEM((images, tokens, width), jnp.bfloat16),
            pltpu.VMEM((1, width), jnp.float32),
            pltpu.VMEM((images, width), jnp.bfloat16),
            weight,
            weight,
            weight,
            weight,
            tall,
            pltpu.VMEM((2, 2, rows, GROUP), jnp.bfloat16),
            pltpu.VMEM((2, rows, GROUP), jnp.bfloat16),
            pltpu.VMEM((2, rows // 2, GROUP), jnp.float32),
            pltpu.VMEM((2, rows // 2, GROUP), jnp.bfloat16),
            pltpu.VMEM((2, images // 4 * GROUP // LANES, tokens, 2 * tokens), jnp.float32),
            pltpu.VMEM((2, images // 4 * GROUP // LANES, 1, 2 * tokens), jnp.float32),
            pltpu.VMEM((images, tokens, LANES), jnp.float32),
            pltpu.VMEM((images * HEADS, width), jnp.bfloat16),
            pltpu.VMEM((images * HEADS, width), jnp.bfloat16),
            pltpu.VMEM((images, width), jnp.float32),
            pltpu.SemaphoreType.DMA((images,)),
            pltpu.SemaphoreType.DMA((2 * width // GROUP,)),
            pltpu.SemaphoreType.DMA((4,)),
        ],
        compiler_params=pltpu.CompilerParams(vmem_limit_bytes=60 * 1024 * 1024),
    )(features, ln_gain.reshape(1, width), w_query, w_key, w_value, w_out, text_raw)


def weigh(logits):
    total = logits.shape[0]
    row_id = lax.broadcasted_iota(jnp.int32, (total, total), 0)
    col_id = lax.broadcasted_iota(jnp.int32, (total, total), 1)
    eye = row_id == col_id
    expo = jnp.exp(logits)
    rowsum = jnp.sum(expo, axis=1, keepdims=True)
    colsum = jnp.sum(expo, axis=0, keepdims=True)
    diag = jnp.sum(jnp.where(eye, logits, 0.0), axis=1, keepdims=True)
    loss = (
        jnp.sum(jnp.log(rowsum) - 2.0 * diag, axis=0, keepdims=True)
        + jnp.sum(jnp.log(colsum), axis=1, keepdims=True)
    ) / (2.0 * total)
    delta = expo * (0.5 / rowsum) + expo * (0.5 / colsum) - jnp.where(eye, 1.0, 0.0)
    return loss, delta.astype(jnp.bfloat16)


def raw_emb_grad(delta, txt, img):
    grad_img = inv_temp * fdot(delta, txt, ((1,), (0,)))
    img32 = img.astype(jnp.float32)
    along = jnp.sum(img32 * grad_img, axis=1, keepdims=True)
    return (grad_img - img32 * along).astype(jnp.bfloat16)


def text_back(text_raw, grad_txt):
    text32 = text_raw.astype(jnp.float32)
    txt_norm = jnp.sqrt(jnp.sum(text32 * text32, axis=1, keepdims=True) + epsilon)
    txt_f = text32 / txt_norm
    return (grad_txt - txt_f * jnp.sum(txt_f * grad_txt, axis=1, keepdims=True)) / txt_norm


def contrast_kernel(
    place_ref,
    all_ref,
    text_hbm,
    loss_hbm,
    text_grad_hbm,
    w_grad_hbm,
    text,
    delta_t,
    loss_out,
    text_grad,
    w_grad,
    sem,
):
    images, width = text.shape
    blocks = width // GROUP
    text_copy = pltpu.make_async_copy(text_hbm, text, sem.at[blocks])
    text_copy.start()
    txt = all_ref[:, 0:width]
    img = all_ref[:, width : 2 * width]
    loss, delta = weigh(inv_temp * fdot(img, txt, ((1,), (1,))))
    loss_out[...] = loss
    copies = [pltpu.make_async_copy(loss_out, loss_hbm, sem.at[blocks + 1])]
    copies[0].start()
    delta_t[...] = jnp.transpose(delta.astype(jnp.float32))
    emb_grad = raw_emb_grad(delta, txt, img)
    own = delta_t[pl.ds(pl.multiple_of(place_ref[0] * images, images), images), :]
    grad_txt = inv_temp * fdot(own.astype(jnp.bfloat16), img, ((1,), (0,)))
    text_copy.wait()
    text_grad[...] = text_back(text[...], grad_txt)
    copies.append(pltpu.make_async_copy(text_grad, text_grad_hbm, sem.at[blocks + 2]))
    copies[1].start()
    for i in range(blocks):
        cols = slice(i * GROUP, (i + 1) * GROUP)
        abn = all_ref[:, 2 * width + i * GROUP : 2 * width + (i + 1) * GROUP]
        w_grad[cols, :] = fdot(abn, emb_grad, ((0,), (0,))).astype(jnp.bfloat16)
        copies.append(pltpu.make_async_copy(w_grad.at[cols], w_grad_hbm.at[cols], sem.at[i]))
        copies[-1].start()
    for c in copies:
        c.wait()


def contrast_call(place, gathered, text_raw):
    total = gathered.shape[0]
    images, width = text_raw.shape
    vmem = pl.BlockSpec(memory_space=pltpu.VMEM)
    hbm = pl.BlockSpec(memory_space=pltpu.HBM)
    return pl.pallas_call(
        contrast_kernel,
        name="contrast",
        out_shape=(
            jax.ShapeDtypeStruct((1, 1), jnp.float32),
            jax.ShapeDtypeStruct((images, width), jnp.float32),
            jax.ShapeDtypeStruct((width, width), jnp.bfloat16),
        ),
        in_specs=[pl.BlockSpec(memory_space=pltpu.SMEM), vmem, hbm],
        out_specs=(hbm, hbm, hbm),
        scratch_shapes=[
            pltpu.VMEM((images, width), jnp.bfloat16),
            pltpu.VMEM((total, total), jnp.float32),
            pltpu.VMEM((1, 1), jnp.float32),
            pltpu.VMEM((images, width), jnp.float32),
            pltpu.VMEM((width, width), jnp.bfloat16),
            pltpu.SemaphoreType.DMA((width // GROUP + 3,)),
        ],
        compiler_params=pltpu.CompilerParams(vmem_limit_bytes=48 * 1024 * 1024),
    )(place, gathered, text_raw)


def stages_of(count):
    bits = count.bit_length() - 1
    stages = []
    low = bits
    while low > 1:
        take = 2 if low > 2 else 1
        low -= take
        stages.append((low, take))
    if bits > 0:
        stages.append((0, 1))
    return stages


def gather(shard, count):
    me = lax.axis_index("dp")
    if count & (count - 1):
        return lax.all_gather(shard, "dp", axis=0, tiled=True), me
    bits = count.bit_length() - 1
    place = jnp.zeros((), jnp.int32)
    held = shard
    weight = 1
    for low, take in stages_of(count):
        size = 1 << take
        digit = (me >> low) & (size - 1)
        block = held.shape[0]
        pieces = [held]
        order = [2, 3, 1] if low + take == bits else [3, 2, 1]
        order = [step for step in order if step < size]
        for step in order:
            pairs = [(i, i ^ (step << low)) for i in range(count)]
            pieces.append(lax.ppermute(held, "dp", pairs))
        joined = jnp.zeros((size * block,) + held.shape[1:], held.dtype)
        for step, piece in zip([0] + order, pieces):
            joined = lax.dynamic_update_slice_in_dim(joined, piece, (digit ^ step) * block, 0)
        held = joined
        place = place + digit * weight
        weight *= size
    return held, place


def local(count, features, ln_gain, w_query, w_key, w_value, w_out, text_raw):
    images, tokens, width = features.shape
    total = images * count
    shard = embed_call(features, ln_gain, w_query, w_key, w_value, w_out, text_raw)
    gathered, place = gather(shard, count)
    if total <= 512:
        loss, text_grad, w_out_grad = contrast_call(place.reshape(1), gathered, text_raw)
    else:
        txt = gathered[:, 0:width]
        img = gathered[:, width : 2 * width]
        abn = gathered[:, 2 * width :]
        loss, delta = weigh(inv_temp * fdot(img, txt, ((1,), (1,))))
        emb_grad = raw_emb_grad(delta, txt, img)
        w_out_grad = fdot(abn, emb_grad, ((0,), (0,)))
        w_out_grad = w_out_grad.astype(jnp.bfloat16)
        own = lax.dynamic_slice_in_dim(delta, place * images, images, 1)
        text_grad = text_back(text_raw, inv_temp * fdot(own, img, ((0,), (0,))))
    return loss.reshape(()), text_grad, w_out_grad


def solution(mesh):
    placed = (P("dp", None, None), P(), P(), P(), P(), P(), P("dp", None))
    return jax.shard_map(
        functools.partial(local, mesh.shape["dp"]),
        mesh=mesh,
        in_specs=placed,
        out_specs=(P(), P("dp", None), P()),
        check_vma=False,
    )
```

```python
import functools

import jax
import jax.numpy as jnp
from jax import lax
from jax.experimental import pallas as pl
from jax.experimental.pallas import tpu as pltpu
from jax.sharding import PartitionSpec as P

HEADS = 16
LANES = 128
GROUP = 256

inv_temp = 1.0 / 0.07
attn_temp = 8.0
epsilon = 1e-06
log2e = 1.4426950408889634


def fdot(a, b, dims):
    return lax.dot_general(a, b, (dims, ((), ())), preferred_element_type=jnp.float32)


def split_bf16(x):
    hi = x.astype(jnp.bfloat16)
    lo = (x - hi.astype(jnp.float32)).astype(jnp.bfloat16)
    return hi, lo


def embed_kernel(
    feat_hbm,
    gain_hbm,
    wq_hbm,
    wk_hbm,
    wv_hbm,
    wo_hbm,
    text_hbm,
    out_ref,
    feat,
    gain_ref,
    text_ref,
    wq,
    wk,
    wv,
    wo,
    normed,
    qn,
    kn,
    raw,
    squared,
    expos,
    scale,
    pooled,
    pn_hi,
    pn_lo,
    xbar,
    feat_sem,
    wqk_sem,
    wvo_sem,
):
    images, tokens, width = feat.shape
    groups = width // GROUP
    head = width // HEADS
    half = images * tokens // 2
    chunk = 16

    feat_copy = [
        pltpu.make_async_copy(feat_hbm.at[b], feat.at[b], feat_sem.at[b]) for b in range(images)
    ]
    wq_copy, wk_copy = [], []
    for g in range(groups):
        cols = pl.ds(g * GROUP, GROUP)
        wq_copy.append(pltpu.make_async_copy(wq_hbm.at[:, cols], wq.at[:, cols], wqk_sem.at[2 * g]))
        wk_copy.append(
            pltpu.make_async_copy(wk_hbm.at[:, cols], wk.at[:, cols], wqk_sem.at[2 * g + 1])
        )
    wv_copy = pltpu.make_async_copy(wv_hbm, wv, wvo_sem.at[0])
    wo_copy = pltpu.make_async_copy(wo_hbm, wo, wvo_sem.at[1])
    gain_copy = pltpu.make_async_copy(gain_hbm, gain_ref, wvo_sem.at[2])
    text_copy = pltpu.make_async_copy(text_hbm, text_ref, wvo_sem.at[3])
    gain_copy.start()
    for b in range(images // 2):
        feat_copy[b].start()
    wq_copy[0].start()
    wk_copy[0].start()
    for b in range(images // 2, images):
        feat_copy[b].start()

    same_head = lax.broadcasted_iota(jnp.int32, (GROUP, GROUP), 0) // head == (
        lax.broadcasted_iota(jnp.int32, (GROUP, GROUP), 1) // head
    )
    block_ones = jnp.where(same_head, 1.0, 0.0).astype(jnp.bfloat16)
    side = lax.rem(lax.broadcasted_iota(jnp.int32, (1, GROUP), 1), LANES) < head
    left = jnp.where(side, 1.0, 0.0).astype(jnp.bfloat16)
    right = jnp.where(side, 0.0, 1.0).astype(jnp.bfloat16)
    share = jnp.where(
        lax.rem(lax.broadcasted_iota(jnp.int32, (1, 2 * tokens), 1), tokens) == 0,
        1.0,
        1.0 / (tokens - 1),
    )

    gain_copy.wait()
    gain = gain_ref[...]

    def normalize(b):
        total = None
        for r in range(0, tokens, chunk):
            x = feat[b, r : r + chunk, :].astype(jnp.float32)
            part = x[0:8, :]
            for i in range(8, chunk, 8):
                part = part + x[i : i + 8, :]
            total = part if total is None else total + part
            center = x - jnp.mean(x, axis=-1, keepdims=True)
            spread = jnp.mean(center * center, axis=-1, keepdims=True)
            normed[b * tokens + r : b * tokens + r + chunk, :] = (
                center * lax.rsqrt(spread + epsilon) * gain
            ).astype(jnp.bfloat16)
        first = feat[b, 0:1, :].astype(jnp.float32)
        total = jnp.sum(total, axis=0, keepdims=True)
        xbar[b : b + 1, :] = first + (total - first) * (1.0 / (tokens - 1))

    head_lane = lax.broadcasted_iota(jnp.int32, (tokens, LANES), 1)
    tiles = GROUP // LANES
    steps = 4 * groups

    def project(k):
        g, part = k // 4, (k % 4) // 2
        w = wq if k % 2 == 0 else wk
        proj = fdot(
            normed[part * half : (part + 1) * half, :],
            w[:, g * GROUP : (g + 1) * GROUP],
            ((1,), (0,)),
        )
        raw[k % 2] = proj
        squared[k % 2] = (proj * proj).astype(jnp.bfloat16)

    def unit(k):
        g, part = k // 4, (k % 4) // 2
        here = slice(part * half, (part + 1) * half)
        squares = fdot(squared[k % 2], block_ones, ((1,), (0,)))
        out = (raw[k % 2] * lax.rsqrt(squares + epsilon)).astype(jnp.bfloat16)
        if k % 2 == 0:
            qn[g % 2, 0, here, :] = out * left
            qn[g % 2, 1, here, :] = out * right
        else:
            kn[g % 2, here, :] = out

    def members(j):
        quarter = images // 4
        for n in range(quarter * tiles):
            yield n, (j % 4) * quarter + n // tiles, n % tiles

    def score(j):
        g = j // 4
        for n, b, t in members(j):
            here = slice(b * tokens, (b + 1) * tokens)
            cols = slice(t * LANES, (t + 1) * LANES)
            stacked = jnp.concatenate([qn[g % 2, 0, here, cols], qn[g % 2, 1, here, cols]], axis=0)
            scores = fdot(kn[g % 2, here, cols], stacked, ((1,), (1,)))
            expo = jnp.exp2(scores * (attn_temp * log2e))
            inverse = share / jnp.sum(expo, axis=0, keepdims=True)
            scale[j % 2, n] = inverse
            expos[j % 2, n] = expo

    def pool(j):
        for n, b, t in members(j):
            weighted = expos[j % 2, n] * scale[j % 2, n]
            h = 2 * ((j // 4) * tiles + t)
            old = pooled[b] if h else jnp.zeros((tokens, LANES), jnp.float32)
            for i in range(2):
                mass = jnp.sum(weighted[:, i * tokens : (i + 1) * tokens], axis=1, keepdims=True)
                old = jnp.where(head_lane == h + i, mass, old)
            pooled[b] = old

    def spread_keys(b):
        hi, lo = split_bf16(jnp.transpose(pooled[b])[0:HEADS, :])
        both = jnp.concatenate([hi, lo], axis=0)
        pn = fdot(both, normed[b * tokens : (b + 1) * tokens, :], ((1,), (0,)))
        hi, lo = split_bf16(pn[0:HEADS, :] + pn[HEADS : 2 * HEADS, :])
        pn_hi[b * HEADS : (b + 1) * HEADS, :] = hi
        pn_lo[b * HEADS : (b + 1) * HEADS, :] = lo

    for b in range(images // 2):
        feat_copy[b].wait()
    wq_copy[1].start()
    wk_copy[1].start()
    for b in range(images // 2):
        normalize(b)
    wq_copy[0].wait()
    wk_copy[0].wait()
    for b in range(images // 2, images):
        feat_copy[b].wait()
    for k in range(steps + 6):
        if k < 2:
            wq_copy[k + 2].start()
            wk_copy[k + 2].start()
        if k == 1:
            text_copy.start()
            wv_copy.start()
            wo_copy.start()
        if k == 4:
            for g in range(1, groups):
                wq_copy[g].wait()
                wk_copy[g].wait()
        if k == 8:
            text_copy.wait()
            wv_copy.wait()
            wo_copy.wait()
        if k < steps:
            project(k)
        if k < 2:
            normalize(images // 2 + 2 * k)
            normalize(images // 2 + 2 * k + 1)
        if 3 <= k < steps + 3:
            score(k - 3)
        if 1 <= k <= steps:
            unit(k - 1)
        if 4 <= k < steps + 4:
            pool(k - 4)
        if k >= steps + 1:
            quarter = images // 4
            for n in range(quarter):
                if k - steps - 1 < 4:
                    spread_keys((k - steps - 1) * quarter + n)

    text32 = text_ref[...].astype(jnp.float32)
    txt_norm = jnp.sqrt(jnp.sum(text32 * text32, axis=1, keepdims=True) + epsilon)
    out_ref[:, 0:width] = (text32 / txt_norm).astype(jnp.bfloat16)

    h_id = lax.broadcasted_iota(jnp.int32, (images, HEADS, GROUP), 1)
    l_id = lax.broadcasted_iota(jnp.int32, (images, HEADS, GROUP), 2) // head
    abar = []
    emb = xbar[...]
    for g in range(groups + 1):
        cols = slice(g * GROUP, (g + 1) * GROUP)
        if g < groups:
            full = fdot(pn_hi[...], wv[:, cols], ((1,), (0,)))
            full = full + fdot(pn_lo[...], wv[:, cols], ((1,), (0,)))
        if g > 0:
            rows = slice((g - 1) * GROUP, g * GROUP)
            emb = emb + fdot(abar[g - 1], wo[rows, :], ((1,), (0,)))
        if g < groups:
            own = h_id == l_id + g * (GROUP // head)
            full = jnp.where(own, full.reshape(images, HEADS, GROUP), 0.0)
            abar.append(jnp.sum(full, axis=1).astype(jnp.bfloat16))
    abar = jnp.concatenate(abar, axis=1)

    emb_norm = jnp.sqrt(jnp.sum(emb * emb, axis=1, keepdims=True) + epsilon)
    out_ref[:, width : 2 * width] = (emb / emb_norm).astype(jnp.bfloat16)
    out_ref[:, 2 * width : 3 * width] = (abar.astype(jnp.float32) / emb_norm).astype(jnp.bfloat16)


def embed_call(features, ln_gain, w_query, w_key, w_value, w_out, text_raw):
    images, tokens, width = features.shape
    rows = images * tokens
    hbm = pl.BlockSpec(memory_space=pltpu.HBM)
    vmem = pl.BlockSpec(memory_space=pltpu.VMEM)
    weight = pltpu.VMEM((width, width), jnp.bfloat16)
    tall = pltpu.VMEM((rows, width), jnp.bfloat16)
    return pl.pallas_call(
        embed_kernel,
        name="embed",
        out_shape=pltpu.VMEM((images, 3 * width), jnp.bfloat16),
        in_specs=[hbm] * 7,
        out_specs=vmem,
        scratch_shapes=[
            pltpu.VMEM((images, tokens, width), jnp.bfloat16),
            pltpu.VMEM((1, width), jnp.float32),
            pltpu.VMEM((images, width), jnp.bfloat16),
            weight,
            weight,
            weight,
            weight,
            tall,
            pltpu.VMEM((2, 2, rows, GROUP), jnp.bfloat16),
            pltpu.VMEM((2, rows, GROUP), jnp.bfloat16),
            pltpu.VMEM((2, rows // 2, GROUP), jnp.float32),
            pltpu.VMEM((2, rows // 2, GROUP), jnp.bfloat16),
            pltpu.VMEM((2, images // 4 * GROUP // LANES, tokens, 2 * tokens), jnp.float32),
            pltpu.VMEM((2, images // 4 * GROUP // LANES, 1, 2 * tokens), jnp.float32),
            pltpu.VMEM((images, tokens, LANES), jnp.float32),
            pltpu.VMEM((images * HEADS, width), jnp.bfloat16),
            pltpu.VMEM((images * HEADS, width), jnp.bfloat16),
            pltpu.VMEM((images, width), jnp.float32),
            pltpu.SemaphoreType.DMA((images,)),
            pltpu.SemaphoreType.DMA((2 * width // GROUP,)),
            pltpu.SemaphoreType.DMA((4,)),
        ],
        compiler_params=pltpu.CompilerParams(vmem_limit_bytes=60 * 1024 * 1024),
    )(features, ln_gain.reshape(1, width), w_query, w_key, w_value, w_out, text_raw)


def weigh(logits):
    total = logits.shape[0]
    row_id = lax.broadcasted_iota(jnp.int32, (total, total), 0)
    col_id = lax.broadcasted_iota(jnp.int32, (total, total), 1)
    eye = row_id == col_id
    expo = jnp.exp(logits)
    rowsum = jnp.sum(expo, axis=1, keepdims=True)
    colsum = jnp.sum(expo, axis=0, keepdims=True)
    diag = jnp.sum(jnp.where(eye, logits, 0.0), axis=1, keepdims=True)
    loss = (
        jnp.sum(jnp.log(rowsum) - 2.0 * diag, axis=0, keepdims=True)
        + jnp.sum(jnp.log(colsum), axis=1, keepdims=True)
    ) / (2.0 * total)
    delta = expo * (0.5 / rowsum) + expo * (0.5 / colsum) - jnp.where(eye, 1.0, 0.0)
    return loss, delta.astype(jnp.bfloat16)


def raw_emb_grad(delta, txt, img):
    grad_img = inv_temp * fdot(delta, txt, ((1,), (0,)))
    img32 = img.astype(jnp.float32)
    along = jnp.sum(img32 * grad_img, axis=1, keepdims=True)
    return (grad_img - img32 * along).astype(jnp.bfloat16)


def text_back(text_raw, grad_txt):
    text32 = text_raw.astype(jnp.float32)
    txt_norm = jnp.sqrt(jnp.sum(text32 * text32, axis=1, keepdims=True) + epsilon)
    txt_f = text32 / txt_norm
    return (grad_txt - txt_f * jnp.sum(txt_f * grad_txt, axis=1, keepdims=True)) / txt_norm


def contrast_kernel(
    place_ref,
    all_ref,
    text_hbm,
    loss_hbm,
    text_grad_hbm,
    w_grad_hbm,
    text,
    delta_t,
    loss_out,
    text_grad,
    w_grad,
    sem,
):
    images, width = text.shape
    blocks = width // GROUP
    text_copy = pltpu.make_async_copy(text_hbm, text, sem.at[blocks])
    text_copy.start()
    txt = all_ref[:, 0:width]
    img = all_ref[:, width : 2 * width]
    loss, delta = weigh(inv_temp * fdot(img, txt, ((1,), (1,))))
    loss_out[...] = loss
    copies = [pltpu.make_async_copy(loss_out, loss_hbm, sem.at[blocks + 1])]
    copies[0].start()
    delta_t[...] = jnp.transpose(delta.astype(jnp.float32))
    emb_grad = raw_emb_grad(delta, txt, img)
    own = delta_t[pl.ds(pl.multiple_of(place_ref[0] * images, images), images), :]
    grad_txt = inv_temp * fdot(own.astype(jnp.bfloat16), img, ((1,), (0,)))
    text_copy.wait()
    text_grad[...] = text_back(text[...], grad_txt)
    copies.append(pltpu.make_async_copy(text_grad, text_grad_hbm, sem.at[blocks + 2]))
    copies[1].start()
    for i in range(blocks):
        cols = slice(i * GROUP, (i + 1) * GROUP)
        abn = all_ref[:, 2 * width + i * GROUP : 2 * width + (i + 1) * GROUP]
        w_grad[cols, :] = fdot(abn, emb_grad, ((0,), (0,))).astype(jnp.bfloat16)
        copies.append(pltpu.make_async_copy(w_grad.at[cols], w_grad_hbm.at[cols], sem.at[i]))
        copies[-1].start()
    for c in copies:
        c.wait()


def contrast_call(place, gathered, text_raw):
    total = gathered.shape[0]
    images, width = text_raw.shape
    vmem = pl.BlockSpec(memory_space=pltpu.VMEM)
    hbm = pl.BlockSpec(memory_space=pltpu.HBM)
    return pl.pallas_call(
        contrast_kernel,
        name="contrast",
        out_shape=(
            jax.ShapeDtypeStruct((1, 1), jnp.float32),
            jax.ShapeDtypeStruct((images, width), jnp.float32),
            jax.ShapeDtypeStruct((width, width), jnp.bfloat16),
        ),
        in_specs=[pl.BlockSpec(memory_space=pltpu.SMEM), vmem, hbm],
        out_specs=(hbm, hbm, hbm),
        scratch_shapes=[
            pltpu.VMEM((images, width), jnp.bfloat16),
            pltpu.VMEM((total, total), jnp.float32),
            pltpu.VMEM((1, 1), jnp.float32),
            pltpu.VMEM((images, width), jnp.float32),
            pltpu.VMEM((width, width), jnp.bfloat16),
            pltpu.SemaphoreType.DMA((width // GROUP + 3,)),
        ],
        compiler_params=pltpu.CompilerParams(vmem_limit_bytes=48 * 1024 * 1024),
    )(place, gathered, text_raw)


def stages_of(count):
    bits = count.bit_length() - 1
    stages = []
    low = bits
    while low > 1:
        take = 2 if low > 2 else 1
        low -= take
        stages.append((low, take))
    if bits > 0:
        stages.append((0, 1))
    return stages


def gather(shard, count):
    me = lax.axis_index("dp")
    if count & (count - 1) or count < 16:
        return lax.all_gather(shard, "dp", axis=0, tiled=True), me

    def swap(block, step, low):
        return lax.ppermute(block, "dp", [(i, i ^ (step << low)) for i in range(count)])

    def put(buffer, block, index):
        return lax.dynamic_update_slice_in_dim(buffer, block, index * block.shape[0], 0)

    stages = stages_of(count)
    rows = shard.shape[0]
    (far, far_take), (near, near_take) = stages[:2]
    fars, nears = 1 << far_take, 1 << near_take
    far_digit, near_digit = (me >> far) & (fars - 1), (me >> near) & (nears - 1)
    far_order = [step for step in (2, 3, 1) if step < fars]
    near_order = [step for step in (3, 2, 1) if step < nears]
    column = {0: shard}
    for step in far_order:
        column[step] = swap(shard, step, far)
    direct = {step: swap(shard, step, near) for step in near_order}
    relay = jnp.concatenate([column[step] for step in range(1, fars)], axis=0)
    relayed = {step: swap(relay, step, near) for step in near_order}
    held = jnp.zeros((fars * nears * rows,) + shard.shape[1:], shard.dtype)
    for n in [0] + near_order:
        for f in range(fars):
            if n == 0:
                block = column[f]
            elif f == 0:
                block = direct[n]
            else:
                block = relayed[n][(f - 1) * rows : f * rows]
            held = put(held, block, (near_digit ^ n) * fars + (far_digit ^ f))
    place = near_digit * fars + far_digit
    weight = fars * nears
    for low, take in stages[2:]:
        size = 1 << take
        digit = (me >> low) & (size - 1)
        order = [step for step in (3, 2, 1) if step < size]
        pieces = [swap(held, step, low) for step in order]
        joined = jnp.zeros((size * held.shape[0],) + held.shape[1:], held.dtype)
        for step, piece in zip([0] + order, [held] + pieces):
            joined = put(joined, piece, digit ^ step)
        held = joined
        place = place + digit * weight
        weight *= size
    return held, place


def local(count, features, ln_gain, w_query, w_key, w_value, w_out, text_raw):
    images, tokens, width = features.shape
    total = images * count
    shard = embed_call(features, ln_gain, w_query, w_key, w_value, w_out, text_raw)
    gathered, place = gather(shard, count)
    if total <= 512:
        loss, text_grad, w_out_grad = contrast_call(place.reshape(1), gathered, text_raw)
    else:
        txt = gathered[:, 0:width]
        img = gathered[:, width : 2 * width]
        abn = gathered[:, 2 * width :]
        loss, delta = weigh(inv_temp * fdot(img, txt, ((1,), (1,))))
        emb_grad = raw_emb_grad(delta, txt, img)
        w_out_grad = fdot(abn, emb_grad, ((0,), (0,)))
        w_out_grad = w_out_grad.astype(jnp.bfloat16)
        own = lax.dynamic_slice_in_dim(delta, place * images, images, 1)
        text_grad = text_back(text_raw, inv_temp * fdot(own, img, ((0,), (0,))))
    return loss.reshape(()), text_grad, w_out_grad


def solution(mesh):
    placed = (P("dp", None, None), P(), P(), P(), P(), P(), P("dp", None))
    return jax.shard_map(
        functools.partial(local, mesh.shape["dp"]),
        mesh=mesh,
        in_specs=placed,
        out_specs=(P(), P("dp", None), P()),
        check_vma=False,
    )
```

```python
import functools

import jax
import jax.numpy as jnp
from jax import lax
from jax.experimental import pallas as pl
from jax.experimental.pallas import tpu as pltpu
from jax.sharding import PartitionSpec as P

HEADS = 16
LANES = 128
GROUP = 256

inv_temp = 1.0 / 0.07
attn_temp = 8.0
epsilon = 1e-06
log2e = 1.4426950408889634


def fdot(a, b, dims):
    return lax.dot_general(a, b, (dims, ((), ())), preferred_element_type=jnp.float32)


def split_bf16(x):
    hi = x.astype(jnp.bfloat16)
    lo = (x - hi.astype(jnp.float32)).astype(jnp.bfloat16)
    return hi, lo


def embed_kernel(
    feat_hbm,
    gain_hbm,
    wq_hbm,
    wk_hbm,
    wv_hbm,
    wo_hbm,
    text_hbm,
    out_ref,
    feat,
    gain_ref,
    text_ref,
    wq,
    wk,
    wv,
    wo,
    normed,
    qn,
    kn,
    raw,
    squared,
    expos,
    scale,
    pooled,
    pn_hi,
    pn_lo,
    xbar,
    feat_sem,
    wqk_sem,
    wvo_sem,
):
    images, tokens, width = feat.shape
    groups = width // GROUP
    head = width // HEADS
    half = images * tokens // 2
    chunk = 16

    feat_copy = [
        pltpu.make_async_copy(feat_hbm.at[b], feat.at[b], feat_sem.at[b]) for b in range(images)
    ]
    wq_copy, wk_copy = [], []
    for g in range(groups):
        cols = pl.ds(g * GROUP, GROUP)
        wq_copy.append(pltpu.make_async_copy(wq_hbm.at[:, cols], wq.at[:, cols], wqk_sem.at[2 * g]))
        wk_copy.append(
            pltpu.make_async_copy(wk_hbm.at[:, cols], wk.at[:, cols], wqk_sem.at[2 * g + 1])
        )
    wv_copy = pltpu.make_async_copy(wv_hbm, wv, wvo_sem.at[0])
    wo_copy = pltpu.make_async_copy(wo_hbm, wo, wvo_sem.at[1])
    gain_copy = pltpu.make_async_copy(gain_hbm, gain_ref, wvo_sem.at[2])
    text_copy = pltpu.make_async_copy(text_hbm, text_ref, wvo_sem.at[3])
    gain_copy.start()
    for b in range(images // 2):
        feat_copy[b].start()
    wq_copy[0].start()
    wk_copy[0].start()
    for b in range(images // 2, images):
        feat_copy[b].start()

    same_head = lax.broadcasted_iota(jnp.int32, (GROUP, GROUP), 0) // head == (
        lax.broadcasted_iota(jnp.int32, (GROUP, GROUP), 1) // head
    )
    block_ones = jnp.where(same_head, 1.0, 0.0).astype(jnp.bfloat16)
    side = lax.rem(lax.broadcasted_iota(jnp.int32, (1, GROUP), 1), LANES) < head
    left = jnp.where(side, 1.0, 0.0).astype(jnp.bfloat16)
    right = jnp.where(side, 0.0, 1.0).astype(jnp.bfloat16)
    share = jnp.where(
        lax.rem(lax.broadcasted_iota(jnp.int32, (1, 2 * tokens), 1), tokens) == 0,
        1.0,
        1.0 / (tokens - 1),
    )

    gain_copy.wait()
    gain = gain_ref[...]

    def normalize(b):
        total = None
        for r in range(0, tokens, chunk):
            x = feat[b, r : r + chunk, :].astype(jnp.float32)
            part = x[0:8, :]
            for i in range(8, chunk, 8):
                part = part + x[i : i + 8, :]
            total = part if total is None else total + part
            center = x - jnp.mean(x, axis=-1, keepdims=True)
            spread = jnp.mean(center * center, axis=-1, keepdims=True)
            normed[b * tokens + r : b * tokens + r + chunk, :] = (
                center * lax.rsqrt(spread + epsilon) * gain
            ).astype(jnp.bfloat16)
        first = feat[b, 0:1, :].astype(jnp.float32)
        total = jnp.sum(total, axis=0, keepdims=True)
        xbar[b : b + 1, :] = first + (total - first) * (1.0 / (tokens - 1))

    head_lane = lax.broadcasted_iota(jnp.int32, (tokens, LANES), 1)
    tiles = GROUP // LANES
    steps = 4 * groups

    def project(k):
        g, part = k // 4, (k % 4) // 2
        w = wq if k % 2 == 0 else wk
        proj = fdot(
            normed[part * half : (part + 1) * half, :],
            w[:, g * GROUP : (g + 1) * GROUP],
            ((1,), (0,)),
        )
        raw[k % 2] = proj
        squared[k % 2] = (proj * proj).astype(jnp.bfloat16)

    def unit(k):
        g, part = k // 4, (k % 4) // 2
        here = slice(part * half, (part + 1) * half)
        squares = fdot(squared[k % 2], block_ones, ((1,), (0,)))
        out = (raw[k % 2] * lax.rsqrt(squares + epsilon)).astype(jnp.bfloat16)
        if k % 2 == 0:
            qn[g % 2, 0, here, :] = out * left
            qn[g % 2, 1, here, :] = out * right
        else:
            kn[g % 2, here, :] = out

    def members(j):
        quarter = images // 4
        for n in range(quarter * tiles):
            yield n, (j % 4) * quarter + n // tiles, n % tiles

    def score(j):
        g = j // 4
        for n, b, t in members(j):
            here = slice(b * tokens, (b + 1) * tokens)
            cols = slice(t * LANES, (t + 1) * LANES)
            stacked = jnp.concatenate([qn[g % 2, 0, here, cols], qn[g % 2, 1, here, cols]], axis=0)
            scores = fdot(kn[g % 2, here, cols], stacked, ((1,), (1,)))
            expo = jnp.exp2(scores * (attn_temp * log2e))
            inverse = share / jnp.sum(expo, axis=0, keepdims=True)
            scale[j % 2, n] = inverse
            expos[j % 2, n] = expo

    def pool(j):
        for n, b, t in members(j):
            weighted = expos[j % 2, n] * scale[j % 2, n]
            h = 2 * ((j // 4) * tiles + t)
            old = pooled[b] if h else jnp.zeros((tokens, LANES), jnp.float32)
            for i in range(2):
                mass = jnp.sum(weighted[:, i * tokens : (i + 1) * tokens], axis=1, keepdims=True)
                old = jnp.where(head_lane == h + i, mass, old)
            pooled[b] = old

    def spread_keys(b):
        hi, lo = split_bf16(jnp.transpose(pooled[b])[0:HEADS, :])
        both = jnp.concatenate([hi, lo], axis=0)
        pn = fdot(both, normed[b * tokens : (b + 1) * tokens, :], ((1,), (0,)))
        hi, lo = split_bf16(pn[0:HEADS, :] + pn[HEADS : 2 * HEADS, :])
        pn_hi[b * HEADS : (b + 1) * HEADS, :] = hi
        pn_lo[b * HEADS : (b + 1) * HEADS, :] = lo

    for b in range(images // 2):
        feat_copy[b].wait()
    wq_copy[1].start()
    wk_copy[1].start()
    for b in range(images // 2):
        normalize(b)
    wq_copy[0].wait()
    wk_copy[0].wait()
    for b in range(images // 2, images):
        feat_copy[b].wait()
    for k in range(steps + 6):
        if k < 2:
            wq_copy[k + 2].start()
            wk_copy[k + 2].start()
        if k == 1:
            text_copy.start()
            wv_copy.start()
            wo_copy.start()
        if k == 4:
            for g in range(1, groups):
                wq_copy[g].wait()
                wk_copy[g].wait()
        if k == 8:
            text_copy.wait()
            wv_copy.wait()
            wo_copy.wait()
        if k < steps:
            project(k)
        if k < 2:
            normalize(images // 2 + 2 * k)
            normalize(images // 2 + 2 * k + 1)
        if 3 <= k < steps + 3:
            score(k - 3)
        if 1 <= k <= steps:
            unit(k - 1)
        if 4 <= k < steps + 4:
            pool(k - 4)
        if k >= steps + 1:
            quarter = images // 4
            for n in range(quarter):
                if k - steps - 1 < 4:
                    spread_keys((k - steps - 1) * quarter + n)

    text32 = text_ref[...].astype(jnp.float32)
    txt_norm = jnp.sqrt(jnp.sum(text32 * text32, axis=1, keepdims=True) + epsilon)
    out_ref[:, 0:width] = (text32 / txt_norm).astype(jnp.bfloat16)

    h_id = lax.broadcasted_iota(jnp.int32, (images, HEADS, GROUP), 1)
    l_id = lax.broadcasted_iota(jnp.int32, (images, HEADS, GROUP), 2) // head
    abar = []
    emb = xbar[...]
    for g in range(groups + 1):
        cols = slice(g * GROUP, (g + 1) * GROUP)
        if g < groups:
            full = fdot(pn_hi[...], wv[:, cols], ((1,), (0,)))
            full = full + fdot(pn_lo[...], wv[:, cols], ((1,), (0,)))
        if g > 0:
            rows = slice((g - 1) * GROUP, g * GROUP)
            emb = emb + fdot(abar[g - 1], wo[rows, :], ((1,), (0,)))
        if g < groups:
            own = h_id == l_id + g * (GROUP // head)
            full = jnp.where(own, full.reshape(images, HEADS, GROUP), 0.0)
            abar.append(jnp.sum(full, axis=1).astype(jnp.bfloat16))
    abar = jnp.concatenate(abar, axis=1)

    emb_norm = jnp.sqrt(jnp.sum(emb * emb, axis=1, keepdims=True) + epsilon)
    out_ref[:, width : 2 * width] = (emb / emb_norm).astype(jnp.bfloat16)
    out_ref[:, 2 * width : 3 * width] = (abar.astype(jnp.float32) / emb_norm).astype(jnp.bfloat16)


def embed_call(features, ln_gain, w_query, w_key, w_value, w_out, text_raw):
    images, tokens, width = features.shape
    rows = images * tokens
    hbm = pl.BlockSpec(memory_space=pltpu.HBM)
    vmem = pl.BlockSpec(memory_space=pltpu.VMEM)
    weight = pltpu.VMEM((width, width), jnp.bfloat16)
    tall = pltpu.VMEM((rows, width), jnp.bfloat16)
    return pl.pallas_call(
        embed_kernel,
        name="embed",
        out_shape=pltpu.VMEM((images, 3 * width), jnp.bfloat16),
        in_specs=[hbm] * 7,
        out_specs=vmem,
        scratch_shapes=[
            pltpu.VMEM((images, tokens, width), jnp.bfloat16),
            pltpu.VMEM((1, width), jnp.float32),
            pltpu.VMEM((images, width), jnp.bfloat16),
            weight,
            weight,
            weight,
            weight,
            tall,
            pltpu.VMEM((2, 2, rows, GROUP), jnp.bfloat16),
            pltpu.VMEM((2, rows, GROUP), jnp.bfloat16),
            pltpu.VMEM((2, rows // 2, GROUP), jnp.float32),
            pltpu.VMEM((2, rows // 2, GROUP), jnp.bfloat16),
            pltpu.VMEM((2, images // 4 * GROUP // LANES, tokens, 2 * tokens), jnp.float32),
            pltpu.VMEM((2, images // 4 * GROUP // LANES, 1, 2 * tokens), jnp.float32),
            pltpu.VMEM((images, tokens, LANES), jnp.float32),
            pltpu.VMEM((images * HEADS, width), jnp.bfloat16),
            pltpu.VMEM((images * HEADS, width), jnp.bfloat16),
            pltpu.VMEM((images, width), jnp.float32),
            pltpu.SemaphoreType.DMA((images,)),
            pltpu.SemaphoreType.DMA((2 * width // GROUP,)),
            pltpu.SemaphoreType.DMA((4,)),
        ],
        compiler_params=pltpu.CompilerParams(vmem_limit_bytes=60 * 1024 * 1024),
    )(features, ln_gain.reshape(1, width), w_query, w_key, w_value, w_out, text_raw)


def weigh(logits):
    total = logits.shape[0]
    row_id = lax.broadcasted_iota(jnp.int32, (total, total), 0)
    col_id = lax.broadcasted_iota(jnp.int32, (total, total), 1)
    eye = row_id == col_id
    expo = jnp.exp(logits)
    rowsum = jnp.sum(expo, axis=1, keepdims=True)
    colsum = jnp.sum(expo, axis=0, keepdims=True)
    diag = jnp.sum(jnp.where(eye, logits, 0.0), axis=1, keepdims=True)
    loss = (
        jnp.sum(jnp.log(rowsum) - 2.0 * diag, axis=0, keepdims=True)
        + jnp.sum(jnp.log(colsum), axis=1, keepdims=True)
    ) / (2.0 * total)
    delta = expo * (0.5 / rowsum) + expo * (0.5 / colsum) - jnp.where(eye, 1.0, 0.0)
    return loss, delta.astype(jnp.bfloat16)


def raw_emb_grad(delta, txt, img):
    grad_img = inv_temp * fdot(delta, txt, ((1,), (0,)))
    img32 = img.astype(jnp.float32)
    along = jnp.sum(img32 * grad_img, axis=1, keepdims=True)
    return (grad_img - img32 * along).astype(jnp.bfloat16)


def text_back(text_raw, grad_txt):
    text32 = text_raw.astype(jnp.float32)
    txt_norm = jnp.sqrt(jnp.sum(text32 * text32, axis=1, keepdims=True) + epsilon)
    txt_f = text32 / txt_norm
    return (grad_txt - txt_f * jnp.sum(txt_f * grad_txt, axis=1, keepdims=True)) / txt_norm


def contrast_kernel(
    place_ref,
    all_ref,
    text_hbm,
    loss_hbm,
    text_grad_hbm,
    w_grad_hbm,
    text,
    delta_t,
    loss_out,
    text_grad,
    w_grad,
    sem,
):
    images, width = text.shape
    blocks = width // GROUP
    text_copy = pltpu.make_async_copy(text_hbm, text, sem.at[blocks])
    text_copy.start()
    txt = all_ref[:, 0:width]
    img = all_ref[:, width : 2 * width]
    loss, delta = weigh(inv_temp * fdot(img, txt, ((1,), (1,))))
    loss_out[...] = loss
    copies = [pltpu.make_async_copy(loss_out, loss_hbm, sem.at[blocks + 1])]
    copies[0].start()
    delta_t[...] = jnp.transpose(delta.astype(jnp.float32))
    emb_grad = raw_emb_grad(delta, txt, img)
    own = delta_t[pl.ds(pl.multiple_of(place_ref[0] * images, images), images), :]
    grad_txt = inv_temp * fdot(own.astype(jnp.bfloat16), img, ((1,), (0,)))
    text_copy.wait()
    text_grad[...] = text_back(text[...], grad_txt)
    copies.append(pltpu.make_async_copy(text_grad, text_grad_hbm, sem.at[blocks + 2]))
    copies[1].start()
    for i in range(blocks):
        cols = slice(i * GROUP, (i + 1) * GROUP)
        abn = all_ref[:, 2 * width + i * GROUP : 2 * width + (i + 1) * GROUP]
        w_grad[cols, :] = fdot(abn, emb_grad, ((0,), (0,))).astype(jnp.bfloat16)
        copies.append(pltpu.make_async_copy(w_grad.at[cols], w_grad_hbm.at[cols], sem.at[i]))
        copies[-1].start()
    for c in copies:
        c.wait()


def contrast_call(place, gathered, text_raw):
    total = gathered.shape[0]
    images, width = text_raw.shape
    vmem = pl.BlockSpec(memory_space=pltpu.VMEM)
    hbm = pl.BlockSpec(memory_space=pltpu.HBM)
    return pl.pallas_call(
        contrast_kernel,
        name="contrast",
        out_shape=(
            jax.ShapeDtypeStruct((1, 1), jnp.float32),
            jax.ShapeDtypeStruct((images, width), jnp.float32),
            jax.ShapeDtypeStruct((width, width), jnp.bfloat16),
        ),
        in_specs=[pl.BlockSpec(memory_space=pltpu.SMEM), vmem, hbm],
        out_specs=(hbm, hbm, hbm),
        scratch_shapes=[
            pltpu.VMEM((images, width), jnp.bfloat16),
            pltpu.VMEM((total, total), jnp.float32),
            pltpu.VMEM((1, 1), jnp.float32),
            pltpu.VMEM((images, width), jnp.float32),
            pltpu.VMEM((width, width), jnp.bfloat16),
            pltpu.SemaphoreType.DMA((width // GROUP + 3,)),
        ],
        compiler_params=pltpu.CompilerParams(vmem_limit_bytes=48 * 1024 * 1024),
    )(place, gathered, text_raw)


def stages_of(count):
    bits = count.bit_length() - 1
    stages = []
    low = bits
    while low > 1:
        take = 2 if low > 2 else 1
        low -= take
        stages.append((low, take))
    if bits > 0:
        stages.append((0, 1))
    return stages


def gather(shard, count):
    me = lax.axis_index("dp")
    if count & (count - 1) or count < 16:
        return lax.all_gather(shard, "dp", axis=0, tiled=True), me

    def swap(block, step, low):
        return lax.ppermute(block, "dp", [(i, i ^ (step << low)) for i in range(count)])

    def put(buffer, block, index):
        return lax.dynamic_update_slice_in_dim(buffer, block, index * block.shape[0], 0)

    stages = stages_of(count)
    rows = shard.shape[0]
    (far, far_take), (near, near_take) = stages[:2]
    fars, nears = 1 << far_take, 1 << near_take
    far_digit, near_digit = (me >> far) & (fars - 1), (me >> near) & (nears - 1)
    far_order = [step for step in (2, 3, 1) if step < fars]
    near_order = [step for step in (3, 2, 1) if step < nears]
    column = {0: shard}
    for step in far_order:
        column[step] = swap(shard, step, far)
    direct = {step: swap(shard, step, near) for step in near_order}
    relay = jnp.concatenate([column[step] for step in far_order], axis=0)
    relayed = {step: swap(relay, step, near) for step in near_order}
    held = jnp.zeros((fars * nears * rows,) + shard.shape[1:], shard.dtype)
    for n in [0] + near_order:
        for f in [0] + far_order:
            if n == 0:
                block = column[f]
            elif f == 0:
                block = direct[n]
            else:
                at = far_order.index(f) * rows
                block = relayed[n][at : at + rows]
            held = put(held, block, (near_digit ^ n) * fars + (far_digit ^ f))
    place = near_digit * fars + far_digit
    weight = fars * nears
    for low, take in stages[2:]:
        size = 1 << take
        digit = (me >> low) & (size - 1)
        order = [step for step in (3, 2, 1) if step < size]
        pieces = [swap(held, step, low) for step in order]
        joined = jnp.zeros((size * held.shape[0],) + held.shape[1:], held.dtype)
        for step, piece in zip([0] + order, [held] + pieces):
            joined = put(joined, piece, digit ^ step)
        held = joined
        place = place + digit * weight
        weight *= size
    return held, place


def local(count, features, ln_gain, w_query, w_key, w_value, w_out, text_raw):
    images, tokens, width = features.shape
    total = images * count
    shard = embed_call(features, ln_gain, w_query, w_key, w_value, w_out, text_raw)
    gathered, place = gather(shard, count)
    if total <= 512:
        loss, text_grad, w_out_grad = contrast_call(place.reshape(1), gathered, text_raw)
    else:
        txt = gathered[:, 0:width]
        img = gathered[:, width : 2 * width]
        abn = gathered[:, 2 * width :]
        loss, delta = weigh(inv_temp * fdot(img, txt, ((1,), (1,))))
        emb_grad = raw_emb_grad(delta, txt, img)
        w_out_grad = fdot(abn, emb_grad, ((0,), (0,)))
        w_out_grad = w_out_grad.astype(jnp.bfloat16)
        own = lax.dynamic_slice_in_dim(delta, place * images, images, 1)
        text_grad = text_back(text_raw, inv_temp * fdot(own, img, ((0,), (0,))))
    return loss.reshape(()), text_grad, w_out_grad


def solution(mesh):
    placed = (P("dp", None, None), P(), P(), P(), P(), P(), P("dp", None))
    return jax.shard_map(
        functools.partial(local, mesh.shape["dp"]),
        mesh=mesh,
        in_specs=placed,
        out_specs=(P(), P("dp", None), P()),
        check_vma=False,
    )
```

```python
import functools

import jax
import jax.numpy as jnp
from jax import lax
from jax.experimental import pallas as pl
from jax.experimental.pallas import tpu as pltpu
from jax.sharding import PartitionSpec as P

HEADS = 16
LANES = 128
GROUP = 256

inv_temp = 1.0 / 0.07
attn_temp = 8.0
epsilon = 1e-06
log2e = 1.4426950408889634


def fdot(a, b, dims):
    return lax.dot_general(a, b, (dims, ((), ())), preferred_element_type=jnp.float32)


def split_bf16(x):
    hi = x.astype(jnp.bfloat16)
    lo = (x - hi.astype(jnp.float32)).astype(jnp.bfloat16)
    return hi, lo


def embed_kernel(
    feat_hbm,
    gain_hbm,
    wq_hbm,
    wk_hbm,
    wv_hbm,
    wo_hbm,
    text_hbm,
    out_ref,
    feat,
    gain_ref,
    text_ref,
    wq,
    wk,
    wv,
    wo,
    normed,
    qn,
    kn,
    raw,
    squared,
    expos,
    scale,
    pooled,
    spread,
    xbar,
    feat_sem,
    wqk_sem,
    wvo_sem,
):
    images, tokens, width = feat.shape
    groups = width // GROUP
    head = width // HEADS
    half = images * tokens // 2
    chunk = 16

    feat_copy = [
        pltpu.make_async_copy(feat_hbm.at[b], feat.at[b], feat_sem.at[b]) for b in range(images)
    ]
    wq_copy, wk_copy = [], []
    for g in range(groups):
        cols = pl.ds(g * GROUP, GROUP)
        wq_copy.append(pltpu.make_async_copy(wq_hbm.at[:, cols], wq.at[:, cols], wqk_sem.at[2 * g]))
        wk_copy.append(
            pltpu.make_async_copy(wk_hbm.at[:, cols], wk.at[:, cols], wqk_sem.at[2 * g + 1])
        )
    wv_copy = pltpu.make_async_copy(wv_hbm, wv, wvo_sem.at[0])
    wo_copy = pltpu.make_async_copy(wo_hbm, wo, wvo_sem.at[1])
    gain_copy = pltpu.make_async_copy(gain_hbm, gain_ref, wvo_sem.at[2])
    text_copy = pltpu.make_async_copy(text_hbm, text_ref, wvo_sem.at[3])
    gain_copy.start()
    for b in range(images // 2):
        feat_copy[b].start()
    wq_copy[0].start()
    wk_copy[0].start()
    for b in range(images // 2, images):
        feat_copy[b].start()

    same_head = lax.broadcasted_iota(jnp.int32, (GROUP, GROUP), 0) // head == (
        lax.broadcasted_iota(jnp.int32, (GROUP, GROUP), 1) // head
    )
    block_ones = jnp.where(same_head, 1.0, 0.0).astype(jnp.bfloat16)
    side = lax.rem(lax.broadcasted_iota(jnp.int32, (1, GROUP), 1), LANES) < head
    left = jnp.where(side, 1.0, 0.0).astype(jnp.bfloat16)
    right = jnp.where(side, 0.0, 1.0).astype(jnp.bfloat16)
    share = jnp.where(
        lax.rem(lax.broadcasted_iota(jnp.int32, (1, 2 * tokens), 1), tokens) == 0,
        1.0,
        1.0 / (tokens - 1),
    )

    gain_copy.wait()
    gain = gain_ref[...]

    def normalize(b):
        total = None
        for r in range(0, tokens, chunk):
            x = feat[b, r : r + chunk, :].astype(jnp.float32)
            part = x[0:8, :]
            for i in range(8, chunk, 8):
                part = part + x[i : i + 8, :]
            total = part if total is None else total + part
            center = x - jnp.mean(x, axis=-1, keepdims=True)
            variance = jnp.mean(center * center, axis=-1, keepdims=True)
            normed[b * tokens + r : b * tokens + r + chunk, :] = (
                center * lax.rsqrt(variance + epsilon) * gain
            ).astype(jnp.bfloat16)
        first = feat[b, 0:1, :].astype(jnp.float32)
        total = jnp.sum(total, axis=0, keepdims=True)
        xbar[b : b + 1, :] = first + (total - first) * (1.0 / (tokens - 1))

    head_lane = lax.broadcasted_iota(jnp.int32, (tokens, LANES), 1)
    tiles = GROUP // LANES
    steps = 4 * groups

    def project(k):
        g, part = k // 4, (k % 4) // 2
        w = wq if k % 2 == 0 else wk
        proj = fdot(
            normed[part * half : (part + 1) * half, :],
            w[:, g * GROUP : (g + 1) * GROUP],
            ((1,), (0,)),
        )
        raw[k % 2] = proj
        squared[k % 2] = (proj * proj).astype(jnp.bfloat16)

    def unit(k):
        g, part = k // 4, (k % 4) // 2
        here = slice(part * half, (part + 1) * half)
        squares = fdot(squared[k % 2], block_ones, ((1,), (0,)))
        out = (raw[k % 2] * lax.rsqrt(squares + epsilon)).astype(jnp.bfloat16)
        if k % 2 == 0:
            qn[g % 2, 0, here, :] = out * left
            qn[g % 2, 1, here, :] = out * right
        else:
            kn[g % 2, here, :] = out

    def members(j):
        quarter = images // 4
        for n in range(quarter * tiles):
            yield n, (j % 4) * quarter + n // tiles, n % tiles

    def score(j):
        g = j // 4
        for n, b, t in members(j):
            here = slice(b * tokens, (b + 1) * tokens)
            cols = slice(t * LANES, (t + 1) * LANES)
            stacked = jnp.concatenate([qn[g % 2, 0, here, cols], qn[g % 2, 1, here, cols]], axis=0)
            scores = fdot(kn[g % 2, here, cols], stacked, ((1,), (1,)))
            expo = jnp.exp2(scores * (attn_temp * log2e))
            inverse = share / jnp.sum(expo, axis=0, keepdims=True)
            scale[j % 2, n] = inverse
            expos[j % 2, n] = expo

    def pool(j):
        for n, b, t in members(j):
            weighted = expos[j % 2, n] * scale[j % 2, n]
            h = 2 * ((j // 4) * tiles + t)
            old = pooled[b] if h else jnp.zeros((tokens, LANES), jnp.float32)
            for i in range(2):
                mass = jnp.sum(weighted[:, i * tokens : (i + 1) * tokens], axis=1, keepdims=True)
                old = jnp.where(head_lane == h + i, mass, old)
            pooled[b] = old

    def spread_keys(b):
        hi, lo = split_bf16(jnp.transpose(pooled[b])[0:HEADS, :])
        both = jnp.concatenate([hi, lo], axis=0)
        pn = fdot(both, normed[b * tokens : (b + 1) * tokens, :], ((1,), (0,)))
        pn = (pn[0:HEADS, :] + pn[HEADS : 2 * HEADS, :]).astype(jnp.bfloat16)
        spread[b * HEADS : (b + 1) * HEADS, :] = pn

    for b in range(images // 2):
        feat_copy[b].wait()
    wq_copy[1].start()
    wk_copy[1].start()
    for b in range(images // 2):
        normalize(b)
    wq_copy[0].wait()
    wk_copy[0].wait()
    for b in range(images // 2, images):
        feat_copy[b].wait()
    for k in range(steps + 6):
        if k < 2:
            wq_copy[k + 2].start()
            wk_copy[k + 2].start()
        if k == 1:
            text_copy.start()
            wv_copy.start()
            wo_copy.start()
        if k == 4:
            for g in range(1, groups):
                wq_copy[g].wait()
                wk_copy[g].wait()
        if k == 8:
            text_copy.wait()
            wv_copy.wait()
            wo_copy.wait()
        if k < steps:
            project(k)
        if k < 2:
            normalize(images // 2 + 2 * k)
            normalize(images // 2 + 2 * k + 1)
        if 3 <= k < steps + 3:
            score(k - 3)
        if 1 <= k <= steps:
            unit(k - 1)
        if 4 <= k < steps + 4:
            pool(k - 4)
        if k >= steps + 1:
            quarter = images // 4
            for n in range(quarter):
                if k - steps - 1 < 4:
                    spread_keys((k - steps - 1) * quarter + n)

    text32 = text_ref[...].astype(jnp.float32)
    txt_norm = jnp.sqrt(jnp.sum(text32 * text32, axis=1, keepdims=True) + epsilon)
    out_ref[:, 0:width] = (text32 / txt_norm).astype(jnp.bfloat16)

    h_id = lax.broadcasted_iota(jnp.int32, (images, HEADS, GROUP), 1)
    l_id = lax.broadcasted_iota(jnp.int32, (images, HEADS, GROUP), 2) // head
    abar = []
    emb = xbar[...]
    for g in range(groups + 1):
        cols = slice(g * GROUP, (g + 1) * GROUP)
        if g < groups:
            full = fdot(spread[...], wv[:, cols], ((1,), (0,)))
        if g > 0:
            rows = slice((g - 1) * GROUP, g * GROUP)
            emb = emb + fdot(abar[g - 1], wo[rows, :], ((1,), (0,)))
        if g < groups:
            own = h_id == l_id + g * (GROUP // head)
            full = jnp.where(own, full.reshape(images, HEADS, GROUP), 0.0)
            abar.append(jnp.sum(full, axis=1).astype(jnp.bfloat16))
    abar = jnp.concatenate(abar, axis=1)

    emb_norm = jnp.sqrt(jnp.sum(emb * emb, axis=1, keepdims=True) + epsilon)
    out_ref[:, width : 2 * width] = (emb / emb_norm).astype(jnp.bfloat16)
    out_ref[:, 2 * width : 3 * width] = (abar.astype(jnp.float32) / emb_norm).astype(jnp.bfloat16)


def embed_call(features, ln_gain, w_query, w_key, w_value, w_out, text_raw):
    images, tokens, width = features.shape
    rows = images * tokens
    hbm = pl.BlockSpec(memory_space=pltpu.HBM)
    vmem = pl.BlockSpec(memory_space=pltpu.VMEM)
    weight = pltpu.VMEM((width, width), jnp.bfloat16)
    tall = pltpu.VMEM((rows, width), jnp.bfloat16)
    return pl.pallas_call(
        embed_kernel,
        name="embed",
        out_shape=pltpu.VMEM((images, 3 * width), jnp.bfloat16),
        in_specs=[hbm] * 7,
        out_specs=vmem,
        scratch_shapes=[
            pltpu.VMEM((images, tokens, width), jnp.bfloat16),
            pltpu.VMEM((1, width), jnp.float32),
            pltpu.VMEM((images, width), jnp.bfloat16),
            weight,
            weight,
            weight,
            weight,
            tall,
            pltpu.VMEM((2, 2, rows, GROUP), jnp.bfloat16),
            pltpu.VMEM((2, rows, GROUP), jnp.bfloat16),
            pltpu.VMEM((2, rows // 2, GROUP), jnp.float32),
            pltpu.VMEM((2, rows // 2, GROUP), jnp.bfloat16),
            pltpu.VMEM((2, images // 4 * GROUP // LANES, tokens, 2 * tokens), jnp.float32),
            pltpu.VMEM((2, images // 4 * GROUP // LANES, 1, 2 * tokens), jnp.float32),
            pltpu.VMEM((images, tokens, LANES), jnp.float32),
            pltpu.VMEM((images * HEADS, width), jnp.bfloat16),
            pltpu.VMEM((images, width), jnp.float32),
            pltpu.SemaphoreType.DMA((images,)),
            pltpu.SemaphoreType.DMA((2 * width // GROUP,)),
            pltpu.SemaphoreType.DMA((4,)),
        ],
        compiler_params=pltpu.CompilerParams(vmem_limit_bytes=60 * 1024 * 1024),
    )(features, ln_gain.reshape(1, width), w_query, w_key, w_value, w_out, text_raw)


def weigh(logits):
    total = logits.shape[0]
    row_id = lax.broadcasted_iota(jnp.int32, (total, total), 0)
    col_id = lax.broadcasted_iota(jnp.int32, (total, total), 1)
    eye = row_id == col_id
    expo = jnp.exp(logits)
    rowsum = jnp.sum(expo, axis=1, keepdims=True)
    colsum = jnp.sum(expo, axis=0, keepdims=True)
    diag = jnp.sum(jnp.where(eye, logits, 0.0), axis=1, keepdims=True)
    loss = (
        jnp.sum(jnp.log(rowsum) - 2.0 * diag, axis=0, keepdims=True)
        + jnp.sum(jnp.log(colsum), axis=1, keepdims=True)
    ) / (2.0 * total)
    delta = expo * (0.5 / rowsum) + expo * (0.5 / colsum) - jnp.where(eye, 1.0, 0.0)
    return loss, delta.astype(jnp.bfloat16)


def raw_emb_grad(delta, txt, img):
    grad_img = inv_temp * fdot(delta, txt, ((1,), (0,)))
    img32 = img.astype(jnp.float32)
    along = jnp.sum(img32 * grad_img, axis=1, keepdims=True)
    return (grad_img - img32 * along).astype(jnp.bfloat16)


def text_back(text_raw, grad_txt):
    text32 = text_raw.astype(jnp.float32)
    txt_norm = jnp.sqrt(jnp.sum(text32 * text32, axis=1, keepdims=True) + epsilon)
    txt_f = text32 / txt_norm
    return (grad_txt - txt_f * jnp.sum(txt_f * grad_txt, axis=1, keepdims=True)) / txt_norm


def contrast_kernel(
    place_ref,
    all_ref,
    text_hbm,
    loss_hbm,
    text_grad_hbm,
    w_grad_hbm,
    text,
    delta_t,
    loss_out,
    text_grad,
    w_grad,
    sem,
):
    images, width = text.shape
    blocks = width // GROUP
    text_copy = pltpu.make_async_copy(text_hbm, text, sem.at[blocks])
    text_copy.start()
    txt = all_ref[:, 0:width]
    img = all_ref[:, width : 2 * width]
    loss, delta = weigh(inv_temp * fdot(img, txt, ((1,), (1,))))
    loss_out[...] = loss
    copies = [pltpu.make_async_copy(loss_out, loss_hbm, sem.at[blocks + 1])]
    copies[0].start()
    delta_t[...] = jnp.transpose(delta.astype(jnp.float32))
    emb_grad = raw_emb_grad(delta, txt, img)
    own = delta_t[pl.ds(pl.multiple_of(place_ref[0] * images, images), images), :]
    grad_txt = inv_temp * fdot(own.astype(jnp.bfloat16), img, ((1,), (0,)))
    text_copy.wait()
    text_grad[...] = text_back(text[...], grad_txt)
    copies.append(pltpu.make_async_copy(text_grad, text_grad_hbm, sem.at[blocks + 2]))
    copies[1].start()
    for i in range(blocks):
        cols = slice(i * GROUP, (i + 1) * GROUP)
        abn = all_ref[:, 2 * width + i * GROUP : 2 * width + (i + 1) * GROUP]
        w_grad[cols, :] = fdot(abn, emb_grad, ((0,), (0,))).astype(jnp.bfloat16)
        copies.append(pltpu.make_async_copy(w_grad.at[cols], w_grad_hbm.at[cols], sem.at[i]))
        copies[-1].start()
    for c in copies:
        c.wait()


def contrast_call(place, gathered, text_raw):
    total = gathered.shape[0]
    images, width = text_raw.shape
    vmem = pl.BlockSpec(memory_space=pltpu.VMEM)
    hbm = pl.BlockSpec(memory_space=pltpu.HBM)
    return pl.pallas_call(
        contrast_kernel,
        name="contrast",
        out_shape=(
            jax.ShapeDtypeStruct((1, 1), jnp.float32),
            jax.ShapeDtypeStruct((images, width), jnp.float32),
            jax.ShapeDtypeStruct((width, width), jnp.bfloat16),
        ),
        in_specs=[pl.BlockSpec(memory_space=pltpu.SMEM), vmem, hbm],
        out_specs=(hbm, hbm, hbm),
        scratch_shapes=[
            pltpu.VMEM((images, width), jnp.bfloat16),
            pltpu.VMEM((total, total), jnp.float32),
            pltpu.VMEM((1, 1), jnp.float32),
            pltpu.VMEM((images, width), jnp.float32),
            pltpu.VMEM((width, width), jnp.bfloat16),
            pltpu.SemaphoreType.DMA((width // GROUP + 3,)),
        ],
        compiler_params=pltpu.CompilerParams(vmem_limit_bytes=48 * 1024 * 1024),
    )(place, gathered, text_raw)


def stages_of(count):
    bits = count.bit_length() - 1
    stages = []
    low = bits
    while low > 1:
        take = 2 if low > 2 else 1
        low -= take
        stages.append((low, take))
    if bits > 0:
        stages.append((0, 1))
    return stages


def gather(shard, count):
    me = lax.axis_index("dp")
    if count & (count - 1) or count < 16:
        return lax.all_gather(shard, "dp", axis=0, tiled=True), me

    def swap(block, step, low):
        return lax.ppermute(block, "dp", [(i, i ^ (step << low)) for i in range(count)])

    def put(buffer, block, index):
        return lax.dynamic_update_slice_in_dim(buffer, block, index * block.shape[0], 0)

    stages = stages_of(count)
    rows = shard.shape[0]
    (far, far_take), (near, near_take) = stages[:2]
    fars, nears = 1 << far_take, 1 << near_take
    far_digit, near_digit = (me >> far) & (fars - 1), (me >> near) & (nears - 1)
    far_order = [step for step in (2, 3, 1) if step < fars]
    near_order = [step for step in (3, 2, 1) if step < nears]
    column = {0: shard}
    for step in far_order:
        column[step] = swap(shard, step, far)
    direct = {step: swap(shard, step, near) for step in near_order}
    relay = jnp.concatenate([column[step] for step in far_order], axis=0)
    relayed = {step: swap(relay, step, near) for step in near_order}
    held = jnp.zeros((fars * nears * rows,) + shard.shape[1:], shard.dtype)
    for n in [0] + near_order:
        for f in [0] + far_order:
            if n == 0:
                block = column[f]
            elif f == 0:
                block = direct[n]
            else:
                at = far_order.index(f) * rows
                block = relayed[n][at : at + rows]
            held = put(held, block, (near_digit ^ n) * fars + (far_digit ^ f))
    place = near_digit * fars + far_digit
    weight = fars * nears
    for low, take in stages[2:]:
        size = 1 << take
        digit = (me >> low) & (size - 1)
        order = [step for step in (3, 2, 1) if step < size]
        pieces = [swap(held, step, low) for step in order]
        joined = jnp.zeros((size * held.shape[0],) + held.shape[1:], held.dtype)
        for step, piece in zip([0] + order, [held] + pieces):
            joined = put(joined, piece, digit ^ step)
        held = joined
        place = place + digit * weight
        weight *= size
    return held, place


def local(count, features, ln_gain, w_query, w_key, w_value, w_out, text_raw):
    images, tokens, width = features.shape
    total = images * count
    shard = embed_call(features, ln_gain, w_query, w_key, w_value, w_out, text_raw)
    gathered, place = gather(shard, count)
    if total <= 512:
        loss, text_grad, w_out_grad = contrast_call(place.reshape(1), gathered, text_raw)
    else:
        txt = gathered[:, 0:width]
        img = gathered[:, width : 2 * width]
        abn = gathered[:, 2 * width :]
        loss, delta = weigh(inv_temp * fdot(img, txt, ((1,), (1,))))
        emb_grad = raw_emb_grad(delta, txt, img)
        w_out_grad = fdot(abn, emb_grad, ((0,), (0,)))
        w_out_grad = w_out_grad.astype(jnp.bfloat16)
        own = lax.dynamic_slice_in_dim(delta, place * images, images, 1)
        text_grad = text_back(text_raw, inv_temp * fdot(own, img, ((0,), (0,))))
    return loss.reshape(()), text_grad, w_out_grad


def solution(mesh):
    placed = (P("dp", None, None), P(), P(), P(), P(), P(), P("dp", None))
    return jax.shard_map(
        functools.partial(local, mesh.shape["dp"]),
        mesh=mesh,
        in_specs=placed,
        out_specs=(P(), P("dp", None), P()),
        check_vma=False,
    )
```

```python
import functools

import jax
import jax.numpy as jnp
from jax import lax
from jax.experimental import pallas as pl
from jax.experimental.pallas import tpu as pltpu
from jax.sharding import PartitionSpec as P

HEADS = 16
LANES = 128
GROUP = 256

inv_temp = 1.0 / 0.07
attn_temp = 8.0
epsilon = 1e-06
log2e = 1.4426950408889634


def fdot(a, b, dims):
    return lax.dot_general(a, b, (dims, ((), ())), preferred_element_type=jnp.float32)


def split_bf16(x):
    hi = x.astype(jnp.bfloat16)
    lo = (x - hi.astype(jnp.float32)).astype(jnp.bfloat16)
    return hi, lo


def embed_kernel(
    feat_hbm,
    gain_hbm,
    wq_hbm,
    wk_hbm,
    wv_hbm,
    wo_hbm,
    text_hbm,
    out_ref,
    feat,
    gain_ref,
    text_ref,
    wq,
    wk,
    wv,
    wo,
    normed,
    qn,
    kn,
    raw,
    squared,
    expos,
    scale,
    pooled,
    spread,
    xbar,
    feat_sem,
    wqk_sem,
    wvo_sem,
):
    images, tokens, width = feat.shape
    groups = width // GROUP
    head = width // HEADS
    half = images * tokens // 2
    chunk = 16

    feat_copy = [
        pltpu.make_async_copy(feat_hbm.at[b], feat.at[b], feat_sem.at[b]) for b in range(images)
    ]
    wq_copy, wk_copy = [], []
    for g in range(groups):
        cols = pl.ds(g * GROUP, GROUP)
        wq_copy.append(pltpu.make_async_copy(wq_hbm.at[:, cols], wq.at[:, cols], wqk_sem.at[2 * g]))
        wk_copy.append(
            pltpu.make_async_copy(wk_hbm.at[:, cols], wk.at[:, cols], wqk_sem.at[2 * g + 1])
        )
    wv_copy = pltpu.make_async_copy(wv_hbm, wv, wvo_sem.at[0])
    wo_copy = pltpu.make_async_copy(wo_hbm, wo, wvo_sem.at[1])
    gain_copy = pltpu.make_async_copy(gain_hbm, gain_ref, wvo_sem.at[2])
    text_copy = pltpu.make_async_copy(text_hbm, text_ref, wvo_sem.at[3])
    gain_copy.start()
    for b in range(images // 2):
        feat_copy[b].start()
    wq_copy[0].start()
    wk_copy[0].start()
    for b in range(images // 2, images):
        feat_copy[b].start()

    same_head = lax.broadcasted_iota(jnp.int32, (GROUP, GROUP), 0) // head == (
        lax.broadcasted_iota(jnp.int32, (GROUP, GROUP), 1) // head
    )
    block_ones = jnp.where(same_head, 1.0, 0.0).astype(jnp.bfloat16)
    side = lax.rem(lax.broadcasted_iota(jnp.int32, (1, GROUP), 1), LANES) < head
    left = jnp.where(side, 1.0, 0.0).astype(jnp.bfloat16)
    right = jnp.where(side, 0.0, 1.0).astype(jnp.bfloat16)
    share = jnp.where(
        lax.rem(lax.broadcasted_iota(jnp.int32, (1, 2 * tokens), 1), tokens) == 0,
        1.0,
        1.0 / (tokens - 1),
    )

    gain_copy.wait()
    gain = gain_ref[...]

    def normalize(b):
        total = None
        for r in range(0, tokens, chunk):
            x = feat[b, r : r + chunk, :].astype(jnp.float32)
            part = x[0:8, :]
            for i in range(8, chunk, 8):
                part = part + x[i : i + 8, :]
            total = part if total is None else total + part
            center = x - jnp.mean(x, axis=-1, keepdims=True)
            variance = jnp.mean(center * center, axis=-1, keepdims=True)
            normed[b * tokens + r : b * tokens + r + chunk, :] = (
                center * lax.rsqrt(variance + epsilon) * gain
            ).astype(jnp.bfloat16)
        first = feat[b, 0:1, :].astype(jnp.float32)
        total = jnp.sum(total, axis=0, keepdims=True)
        xbar[b : b + 1, :] = first + (total - first) * (1.0 / (tokens - 1))

    head_lane = lax.broadcasted_iota(jnp.int32, (tokens, LANES), 1)
    tiles = GROUP // LANES
    steps = 4 * groups

    def project(k):
        g, part = k // 4, (k % 4) // 2
        w = wq if k % 2 == 0 else wk
        proj = fdot(
            normed[part * half : (part + 1) * half, :],
            w[:, g * GROUP : (g + 1) * GROUP],
            ((1,), (0,)),
        )
        raw[k % 2] = proj
        squared[k % 2] = (proj * proj).astype(jnp.bfloat16)

    def unit(k):
        g, part = k // 4, (k % 4) // 2
        here = slice(part * half, (part + 1) * half)
        squares = fdot(squared[k % 2], block_ones, ((1,), (0,)))
        factor = attn_temp * log2e if k % 2 == 0 else 1.0
        out = (raw[k % 2] * (lax.rsqrt(squares + epsilon) * factor)).astype(jnp.bfloat16)
        if k % 2 == 0:
            qn[g % 2, 0, here, :] = out * left
            qn[g % 2, 1, here, :] = out * right
        else:
            kn[g % 2, here, :] = out

    def members(j):
        quarter = images // 4
        for n in range(quarter * tiles):
            yield n, (j % 4) * quarter + n // tiles, n % tiles

    def score(j):
        g = j // 4
        for n, b, t in members(j):
            here = slice(b * tokens, (b + 1) * tokens)
            cols = slice(t * LANES, (t + 1) * LANES)
            stacked = jnp.concatenate([qn[g % 2, 0, here, cols], qn[g % 2, 1, here, cols]], axis=0)
            scores = fdot(kn[g % 2, here, cols], stacked, ((1,), (1,)))
            expo = jnp.exp2(scores)
            inverse = share / jnp.sum(expo, axis=0, keepdims=True)
            scale[j % 2, n] = inverse
            expos[j % 2, n] = expo

    def pool(j):
        for n, b, t in members(j):
            weighted = expos[j % 2, n] * scale[j % 2, n]
            h = 2 * ((j // 4) * tiles + t)
            old = pooled[b] if h else jnp.zeros((tokens, LANES), jnp.float32)
            for i in range(2):
                mass = jnp.sum(weighted[:, i * tokens : (i + 1) * tokens], axis=1, keepdims=True)
                old = jnp.where(head_lane == h + i, mass, old)
            pooled[b] = old

    def spread_keys(b):
        hi, lo = split_bf16(jnp.transpose(pooled[b])[0:HEADS, :])
        both = jnp.concatenate([hi, lo], axis=0)
        pn = fdot(both, normed[b * tokens : (b + 1) * tokens, :], ((1,), (0,)))
        pn = (pn[0:HEADS, :] + pn[HEADS : 2 * HEADS, :]).astype(jnp.bfloat16)
        spread[b * HEADS : (b + 1) * HEADS, :] = pn

    for b in range(images // 2):
        feat_copy[b].wait()
    wq_copy[1].start()
    wk_copy[1].start()
    for b in range(images // 2):
        normalize(b)
    wq_copy[0].wait()
    wk_copy[0].wait()
    for b in range(images // 2, images):
        feat_copy[b].wait()
    for k in range(steps + 6):
        if k < 2:
            wq_copy[k + 2].start()
            wk_copy[k + 2].start()
        if k == 1:
            text_copy.start()
            wv_copy.start()
            wo_copy.start()
        if k == 4:
            for g in range(1, groups):
                wq_copy[g].wait()
                wk_copy[g].wait()
        if k == 8:
            text_copy.wait()
            wv_copy.wait()
            wo_copy.wait()
        if k < steps:
            project(k)
        if k < 2:
            normalize(images // 2 + 2 * k)
            normalize(images // 2 + 2 * k + 1)
        if 3 <= k < steps + 3:
            score(k - 3)
        if 1 <= k <= steps:
            unit(k - 1)
        if 4 <= k < steps + 4:
            pool(k - 4)
        if k >= steps + 1:
            quarter = images // 4
            for n in range(quarter):
                if k - steps - 1 < 4:
                    spread_keys((k - steps - 1) * quarter + n)

    text32 = text_ref[...].astype(jnp.float32)
    txt_norm = jnp.sqrt(jnp.sum(text32 * text32, axis=1, keepdims=True) + epsilon)
    out_ref[:, 0:width] = (text32 / txt_norm).astype(jnp.bfloat16)

    h_id = lax.broadcasted_iota(jnp.int32, (images, HEADS, GROUP), 1)
    l_id = lax.broadcasted_iota(jnp.int32, (images, HEADS, GROUP), 2) // head
    abar = []
    emb = xbar[...]
    for g in range(groups + 1):
        cols = slice(g * GROUP, (g + 1) * GROUP)
        if g < groups:
            full = fdot(spread[...], wv[:, cols], ((1,), (0,)))
        if g > 0:
            rows = slice((g - 1) * GROUP, g * GROUP)
            emb = emb + fdot(abar[g - 1], wo[rows, :], ((1,), (0,)))
        if g < groups:
            own = h_id == l_id + g * (GROUP // head)
            full = jnp.where(own, full.reshape(images, HEADS, GROUP), 0.0)
            abar.append(jnp.sum(full, axis=1).astype(jnp.bfloat16))
    abar = jnp.concatenate(abar, axis=1)

    emb_norm = jnp.sqrt(jnp.sum(emb * emb, axis=1, keepdims=True) + epsilon)
    out_ref[:, width : 2 * width] = (emb / emb_norm).astype(jnp.bfloat16)
    out_ref[:, 2 * width : 3 * width] = (abar.astype(jnp.float32) / emb_norm).astype(jnp.bfloat16)


def embed_call(features, ln_gain, w_query, w_key, w_value, w_out, text_raw):
    images, tokens, width = features.shape
    rows = images * tokens
    hbm = pl.BlockSpec(memory_space=pltpu.HBM)
    vmem = pl.BlockSpec(memory_space=pltpu.VMEM)
    weight = pltpu.VMEM((width, width), jnp.bfloat16)
    tall = pltpu.VMEM((rows, width), jnp.bfloat16)
    return pl.pallas_call(
        embed_kernel,
        name="embed",
        out_shape=pltpu.VMEM((images, 3 * width), jnp.bfloat16),
        in_specs=[hbm] * 7,
        out_specs=vmem,
        scratch_shapes=[
            pltpu.VMEM((images, tokens, width), jnp.bfloat16),
            pltpu.VMEM((1, width), jnp.float32),
            pltpu.VMEM((images, width), jnp.bfloat16),
            weight,
            weight,
            weight,
            weight,
            tall,
            pltpu.VMEM((2, 2, rows, GROUP), jnp.bfloat16),
            pltpu.VMEM((2, rows, GROUP), jnp.bfloat16),
            pltpu.VMEM((2, rows // 2, GROUP), jnp.float32),
            pltpu.VMEM((2, rows // 2, GROUP), jnp.bfloat16),
            pltpu.VMEM((2, images // 4 * GROUP // LANES, tokens, 2 * tokens), jnp.float32),
            pltpu.VMEM((2, images // 4 * GROUP // LANES, 1, 2 * tokens), jnp.float32),
            pltpu.VMEM((images, tokens, LANES), jnp.float32),
            pltpu.VMEM((images * HEADS, width), jnp.bfloat16),
            pltpu.VMEM((images, width), jnp.float32),
            pltpu.SemaphoreType.DMA((images,)),
            pltpu.SemaphoreType.DMA((2 * width // GROUP,)),
            pltpu.SemaphoreType.DMA((4,)),
        ],
        compiler_params=pltpu.CompilerParams(vmem_limit_bytes=60 * 1024 * 1024),
    )(features, ln_gain.reshape(1, width), w_query, w_key, w_value, w_out, text_raw)


def weigh(logits):
    total = logits.shape[0]
    row_id = lax.broadcasted_iota(jnp.int32, (total, total), 0)
    col_id = lax.broadcasted_iota(jnp.int32, (total, total), 1)
    eye = row_id == col_id
    expo = jnp.exp(logits)
    rowsum = jnp.sum(expo, axis=1, keepdims=True)
    colsum = jnp.sum(expo, axis=0, keepdims=True)
    diag = jnp.sum(jnp.where(eye, logits, 0.0), axis=1, keepdims=True)
    loss = (
        jnp.sum(jnp.log(rowsum) - 2.0 * diag, axis=0, keepdims=True)
        + jnp.sum(jnp.log(colsum), axis=1, keepdims=True)
    ) / (2.0 * total)
    delta = expo * (0.5 / rowsum) + expo * (0.5 / colsum) - jnp.where(eye, 1.0, 0.0)
    return loss, delta.astype(jnp.bfloat16)


def raw_emb_grad(delta, txt, img):
    grad_img = inv_temp * fdot(delta, txt, ((1,), (0,)))
    img32 = img.astype(jnp.float32)
    along = jnp.sum(img32 * grad_img, axis=1, keepdims=True)
    return (grad_img - img32 * along).astype(jnp.bfloat16)


def text_back(text_raw, grad_txt):
    text32 = text_raw.astype(jnp.float32)
    txt_norm = jnp.sqrt(jnp.sum(text32 * text32, axis=1, keepdims=True) + epsilon)
    txt_f = text32 / txt_norm
    return (grad_txt - txt_f * jnp.sum(txt_f * grad_txt, axis=1, keepdims=True)) / txt_norm


def contrast_kernel(
    place_ref,
    all_ref,
    text_hbm,
    loss_hbm,
    text_grad_hbm,
    w_grad_hbm,
    text,
    delta_t,
    loss_out,
    text_grad,
    w_grad,
    sem,
):
    images, width = text.shape
    blocks = width // GROUP
    text_copy = pltpu.make_async_copy(text_hbm, text, sem.at[blocks])
    text_copy.start()
    txt = all_ref[:, 0:width]
    img = all_ref[:, width : 2 * width]
    loss, delta = weigh(inv_temp * fdot(img, txt, ((1,), (1,))))
    loss_out[...] = loss
    copies = [pltpu.make_async_copy(loss_out, loss_hbm, sem.at[blocks + 1])]
    copies[0].start()
    delta_t[...] = jnp.transpose(delta.astype(jnp.float32))
    emb_grad = raw_emb_grad(delta, txt, img)
    own = delta_t[pl.ds(pl.multiple_of(place_ref[0] * images, images), images), :]
    grad_txt = inv_temp * fdot(own.astype(jnp.bfloat16), img, ((1,), (0,)))
    text_copy.wait()
    text_grad[...] = text_back(text[...], grad_txt)
    copies.append(pltpu.make_async_copy(text_grad, text_grad_hbm, sem.at[blocks + 2]))
    copies[1].start()
    for i in range(blocks):
        cols = slice(i * GROUP, (i + 1) * GROUP)
        abn = all_ref[:, 2 * width + i * GROUP : 2 * width + (i + 1) * GROUP]
        w_grad[cols, :] = fdot(abn, emb_grad, ((0,), (0,))).astype(jnp.bfloat16)
        copies.append(pltpu.make_async_copy(w_grad.at[cols], w_grad_hbm.at[cols], sem.at[i]))
        copies[-1].start()
    for c in copies:
        c.wait()


def contrast_call(place, gathered, text_raw):
    total = gathered.shape[0]
    images, width = text_raw.shape
    vmem = pl.BlockSpec(memory_space=pltpu.VMEM)
    hbm = pl.BlockSpec(memory_space=pltpu.HBM)
    return pl.pallas_call(
        contrast_kernel,
        name="contrast",
        out_shape=(
            jax.ShapeDtypeStruct((1, 1), jnp.float32),
            jax.ShapeDtypeStruct((images, width), jnp.float32),
            jax.ShapeDtypeStruct((width, width), jnp.bfloat16),
        ),
        in_specs=[pl.BlockSpec(memory_space=pltpu.SMEM), vmem, hbm],
        out_specs=(hbm, hbm, hbm),
        scratch_shapes=[
            pltpu.VMEM((images, width), jnp.bfloat16),
            pltpu.VMEM((total, total), jnp.float32),
            pltpu.VMEM((1, 1), jnp.float32),
            pltpu.VMEM((images, width), jnp.float32),
            pltpu.VMEM((width, width), jnp.bfloat16),
            pltpu.SemaphoreType.DMA((width // GROUP + 3,)),
        ],
        compiler_params=pltpu.CompilerParams(vmem_limit_bytes=48 * 1024 * 1024),
    )(place, gathered, text_raw)


def stages_of(count):
    bits = count.bit_length() - 1
    stages = []
    low = bits
    while low > 1:
        take = 2 if low > 2 else 1
        low -= take
        stages.append((low, take))
    if bits > 0:
        stages.append((0, 1))
    return stages


def gather(shard, count):
    me = lax.axis_index("dp")
    if count & (count - 1) or count < 16:
        return lax.all_gather(shard, "dp", axis=0, tiled=True), me

    def swap(block, step, low):
        return lax.ppermute(block, "dp", [(i, i ^ (step << low)) for i in range(count)])

    def put(buffer, block, index):
        return lax.dynamic_update_slice_in_dim(buffer, block, index * block.shape[0], 0)

    stages = stages_of(count)
    rows = shard.shape[0]
    (far, far_take), (near, near_take) = stages[:2]
    fars, nears = 1 << far_take, 1 << near_take
    far_digit, near_digit = (me >> far) & (fars - 1), (me >> near) & (nears - 1)
    far_order = [step for step in (2, 3, 1) if step < fars]
    near_order = [step for step in (3, 2, 1) if step < nears]
    column = {0: shard}
    for step in far_order:
        column[step] = swap(shard, step, far)
    direct = {step: swap(shard, step, near) for step in near_order}
    relay = jnp.concatenate([column[step] for step in far_order], axis=0)
    relayed = {step: swap(relay, step, near) for step in near_order}
    held = jnp.zeros((fars * nears * rows,) + shard.shape[1:], shard.dtype)
    for n in [0] + near_order:
        for f in [0] + far_order:
            if n == 0:
                block = column[f]
            elif f == 0:
                block = direct[n]
            else:
                at = far_order.index(f) * rows
                block = relayed[n][at : at + rows]
            held = put(held, block, (near_digit ^ n) * fars + (far_digit ^ f))
    place = near_digit * fars + far_digit
    weight = fars * nears
    for low, take in stages[2:]:
        size = 1 << take
        digit = (me >> low) & (size - 1)
        order = [step for step in (3, 2, 1) if step < size]
        pieces = [swap(held, step, low) for step in order]
        joined = jnp.zeros((size * held.shape[0],) + held.shape[1:], held.dtype)
        for step, piece in zip([0] + order, [held] + pieces):
            joined = put(joined, piece, digit ^ step)
        held = joined
        place = place + digit * weight
        weight *= size
    return held, place


def local(count, features, ln_gain, w_query, w_key, w_value, w_out, text_raw):
    images, tokens, width = features.shape
    total = images * count
    shard = embed_call(features, ln_gain, w_query, w_key, w_value, w_out, text_raw)
    gathered, place = gather(shard, count)
    if total <= 512:
        loss, text_grad, w_out_grad = contrast_call(place.reshape(1), gathered, text_raw)
    else:
        txt = gathered[:, 0:width]
        img = gathered[:, width : 2 * width]
        abn = gathered[:, 2 * width :]
        loss, delta = weigh(inv_temp * fdot(img, txt, ((1,), (1,))))
        emb_grad = raw_emb_grad(delta, txt, img)
        w_out_grad = fdot(abn, emb_grad, ((0,), (0,)))
        w_out_grad = w_out_grad.astype(jnp.bfloat16)
        own = lax.dynamic_slice_in_dim(delta, place * images, images, 1)
        text_grad = text_back(text_raw, inv_temp * fdot(own, img, ((0,), (0,))))
    return loss.reshape(()), text_grad, w_out_grad


def solution(mesh):
    placed = (P("dp", None, None), P(), P(), P(), P(), P(), P("dp", None))
    return jax.shard_map(
        functools.partial(local, mesh.shape["dp"]),
        mesh=mesh,
        in_specs=placed,
        out_specs=(P(), P("dp", None), P()),
        check_vma=False,
    )
```
